256 devices in a mesh: seq: 16 (over y, x), grp: 16 (over z, core).
Axes of the slice: x: 4, y: 4, z: 8, core: 2. Of those that a mesh axis runs over, the one named last changes fastest.
Arguments:
- actions: int32 [32, 7], P('grp'), may hold values from 0 to 255
- lengths: int32 [32], P('grp'), may hold values from 2048 to 4096
- embed: bfloat16 [256, 4096], replicated, may hold values from -6 to 6
- attn_gain: float32 [4096], replicated, may hold values from 0.1 to 1.9
- w_query: bfloat16 [4096, 4096], P('grp', 'seq'), may hold values from -0.09375 to 0.09375
- w_key: bfloat16 [4096, 4096], P('grp', 'seq'), may hold values from -0.140625 to 0.140625
- w_value: bfloat16 [4096, 4096], P('grp', 'seq'), may hold values from -0.09375 to 0.09375
- w_out: bfloat16 [4096, 4096], P('grp', 'seq'), may hold values from -0.09375 to 0.09375
- key_cache: bfloat16 [32, 4096, 4096], P('grp', 'seq'), may hold values from -136 to 136
- value_cache: bfloat16 [32, 4096, 4096], P('grp', 'seq'), may hold values from -6 to 6
- final_gain: float32 [4096], replicated, may hold values from 0.1 to 1.9
- head: bfloat16 [256, 4096], P('seq'), may hold values from -0.25 to 0.25
Outputs:
- logprob: float32 [32, 7, 256], P('grp', None, 'seq')
The draws below stay inside these ranges and needn't reach their ends.
Inputs may be any that keep to these rules, and one draw needn't show every extreme that they name: Robot r's prompt occupies cache positions 0 to lengths[r] - 1.
All inputs are finite; a program needn't handle non-finite values.
Results may differ from the reference program's by a relative error of at most 0.008.
Values may be sent and summed in bfloat16 or wider, within the bound.
No kernel may reach another device: no remote copies, remote signals or barrier semaphores. Data moves between devices by JAX's collectives and lax.ppermute only.
A program may use at most 64 MiB of HBM per device.

```python
import jax
import jax.numpy as jnp
from jax import lax

D = 4096
HEADS = 32
HEAD_DIM = 128
BINS = 256
STEPS = 7
ROBOTS = 32
PROMPT = 4096


def projection_pair(key):
    first, second = jax.random.split(jax.random.fold_in(key, 29), 2)
    scale = D ** (-0.5)
    query_part = jnp.clip(jax.random.normal(first, (D, D), jnp.float32), -6.0, 6.0) * scale
    noise_part = jnp.clip(jax.random.normal(second, (D, D), jnp.float32), -6.0, 6.0) * scale
    key_part = 0.75 * query_part + 0.66 * noise_part
    return (query_part, key_part)


def draw_w_query(key, part):
    query_part, key_part = projection_pair(key)
    return query_part.astype(jnp.bfloat16)


def draw_w_key(key, part):
    query_part, key_part = projection_pair(key)
    return key_part.astype(jnp.bfloat16)


def draw_key_cache(key, part):
    first = jax.random.fold_in(jax.random.fold_in(key, 17), 0)
    base = jnp.clip(jax.random.normal(first, (ROBOTS, PROMPT, D), jnp.float32), -6.0, 6.0)
    return base.astype(jnp.bfloat16)


def touch_ends(result, own_key, low, high):
    dims = result.shape
    place = [jax.random.randint(jax.random.fold_in(own_key, axis), (), 0, dims[axis]) for axis in range(len(dims))]
    result = result.at[tuple(place)].set(low)
    longest = dims.index(max(dims))
    place[longest] = (place[longest] + 1) % dims[longest]
    return result.at[tuple(place)].set(high)


def level_of(own_key, extent, cuts, smallest, high):
    factor_of = 1.0
    for dim, shards_of in cuts:
        heights = jax.random.uniform(jax.random.fold_in(jax.random.fold_in(own_key, 6), dim), (shards_of,), jnp.float32, smallest / len(cuts), high / len(cuts))
        factor_of = factor_of * jnp.repeat(jnp.exp(heights), extent[dim] // shards_of).reshape((-1,) + (1,) * (len(extent) - 1 - dim))
    return factor_of


def normal_values(own_key, dims, width, limit, cuts=(), kind=jnp.bfloat16):
    level = level_of(own_key, dims, cuts, -0.22, 0.18) if cuts else 1.0
    entries = jax.random.normal(own_key, dims, jnp.float32) * width * level
    return jnp.minimum(jnp.maximum(entries, -limit), limit).astype(kind)


def setup_inputs(seed: int = 0) -> dict:
    splits = jax.random.split(jax.random.key(seed), 13)
    actions = touch_ends(jax.random.randint(splits[0], (ROBOTS, STEPS), 0, BINS), jax.random.fold_in(splits[0], 1), 0, BINS - 1).astype(jnp.int32)
    lengths = touch_ends(jax.random.randint(splits[1], (ROBOTS,), PROMPT // 2, PROMPT + 1), jax.random.fold_in(splits[1], 1), PROMPT // 2, PROMPT).astype(jnp.int32)
    embed = normal_values(splits[2], (BINS, D), 1.0, 6.0)
    attn_gain = jnp.clip(1.0 + 0.18 * jax.random.normal(splits[3], (D,), jnp.float32), 0.1, 1.9)
    w_query = draw_w_query(jax.random.fold_in(splits[12], 71), 0)
    w_key = draw_w_key(jax.random.fold_in(splits[12], 71), 0)
    w_value = normal_values(splits[6], (D, D), D ** -0.5, 0.09375, ((0, 16), (1, 16)))
    w_out = normal_values(splits[7], (D, D), D ** -0.5, 0.09375, ((0, 16), (1, 16)))
    key_cache = draw_key_cache(jax.random.fold_in(splits[12], 71), 0)
    value_cache = normal_values(splits[9], (ROBOTS, PROMPT, D), 1.0, 6.0, ((0, 16), (1, 16)))
    final_gain = jnp.clip(1.0 + 0.18 * jax.random.normal(splits[10], (D,), jnp.float32), 0.1, 1.9)
    head = normal_values(splits[11], (BINS, D), (D // 9) ** -0.5, 0.25, ((0, 16),))
    return dict(actions=actions, lengths=lengths, embed=embed, attn_gain=attn_gain, w_query=w_query, w_key=w_key, w_value=w_value, w_out=w_out, key_cache=key_cache, value_cache=value_cache, final_gain=final_gain, head=head)


def rms_scale(values, gain):
    mean_square = lax.optimization_barrier(jnp.mean(values * values, axis=-1, keepdims=True))
    return values * lax.rsqrt(mean_square + 1e-05) * gain

def rotate(values, places):
    half = values.shape[-1] // 2
    freq = 10000.0 ** (-(jnp.arange(half, dtype=jnp.float32) * 2.0 / values.shape[-1]))
    angle = places[..., None, None] * freq
    first = values[..., :half]
    second = values[..., half:]
    cosine = jnp.cos(angle)
    sine = jnp.sin(angle)
    return jnp.concatenate([first * cosine - second * sine, second * cosine + first * sine], axis=-1)

def reference(actions, lengths, embed, attn_gain, w_query, w_key, w_value, w_out, key_cache, value_cache, final_gain, head):
    bins = jnp.arange(BINS, dtype=jnp.int32)
    onehot = (actions[:, :, None] == bins[None, None, :]).astype(jnp.float32)
    inputs = jnp.einsum('rtb,bd->rtd', onehot, embed.astype(jnp.float32))
    normed = rms_scale(inputs, attn_gain).astype(jnp.bfloat16).reshape(ROBOTS * STEPS, D)
    places = (lengths[:, None] + jnp.arange(STEPS, dtype=jnp.int32)[None, :]).astype(jnp.float32)

    def heads_of(flat):
        return flat.reshape(ROBOTS, STEPS, HEADS, HEAD_DIM)
    query = rotate(heads_of(jnp.dot(normed, w_query, preferred_element_type=jnp.float32)), places).astype(jnp.bfloat16)
    key = rotate(heads_of(jnp.dot(normed, w_key, preferred_element_type=jnp.float32)), places).astype(jnp.bfloat16)
    value = heads_of(jnp.dot(normed, w_value, preferred_element_type=jnp.float32)).astype(jnp.bfloat16)
    scale = HEAD_DIM ** (-0.5)
    prompt_index = jnp.arange(PROMPT, dtype=jnp.int32)
    step_index = jnp.arange(STEPS, dtype=jnp.int32)
    causal = step_index[None, :] <= step_index[:, None]

    def one_robot(items):
        query_r, key_r, value_r, cache_k, cache_v, length = items
        query_f = query_r.astype(jnp.float32)
        cache_k = cache_k.reshape(PROMPT, HEADS, HEAD_DIM).astype(jnp.float32)
        cache_v = cache_v.reshape(PROMPT, HEADS, HEAD_DIM).astype(jnp.float32)
        valid = prompt_index < length
        prompt_scores = jnp.einsum('thd,phd->thp', query_f, cache_k) * scale
        window_scores = jnp.einsum('thd,jhd->thj', query_f, key_r.astype(jnp.float32)) * scale
        prompt_scores = jnp.where(valid[None, None, :], prompt_scores, -1e+30)
        window_scores = jnp.where(causal[:, None, :], window_scores, -1e+30)
        top = jnp.maximum(lax.optimization_barrier(jnp.max(prompt_scores, axis=-1)), lax.optimization_barrier(jnp.max(window_scores, axis=-1)))
        prompt_e = jnp.where(valid[None, None, :], jnp.exp(prompt_scores - top[..., None]), 0.0)
        window_e = jnp.where(causal[:, None, :], jnp.exp(window_scores - top[..., None]), 0.0)
        total = lax.optimization_barrier(jnp.sum(prompt_e, axis=-1)) + lax.optimization_barrier(jnp.sum(window_e, axis=-1))
        prompt_p = prompt_e.astype(jnp.bfloat16).astype(jnp.float32)
        window_p = window_e.astype(jnp.bfloat16).astype(jnp.float32)
        acc = jnp.einsum('thp,phd->thd', prompt_p, cache_v) + jnp.einsum('thj,jhd->thd', window_p, value_r.astype(jnp.float32))
        return (acc / total[..., None]).astype(jnp.bfloat16).reshape(STEPS, D)
    attended = lax.map(one_robot, (query, key, value, key_cache, value_cache, lengths))
    branch = jnp.dot(attended.reshape(ROBOTS * STEPS, D), w_out, preferred_element_type=jnp.float32)
    residual = inputs.reshape(ROBOTS * STEPS, D) + branch
    final = rms_scale(residual, final_gain).astype(jnp.bfloat16)
    logits = jnp.dot(final, head.T, preferred_element_type=jnp.float32)
    top = lax.optimization_barrier(jnp.max(logits, axis=-1, keepdims=True))
    logprob = logits - top - jnp.log(lax.optimization_barrier(jnp.sum(jnp.exp(logits - top), axis=-1, keepdims=True)))
    return logprob.reshape(ROBOTS, STEPS, BINS)
```

```python
import jax
import jax.numpy as jnp
from jax import lax
from jax.sharding import Mesh
from jax.sharding import PartitionSpec as P

HEAD_DIM = 128
SEQ = ("seq_0", "seq_1")
GRP = ("z", "core")
NEG = -1e30


def exchange(pieces, axis):
    return lax.all_to_all(pieces, axis, split_axis=0, concat_axis=0, tiled=True)


def copy_for_each(shard, axis):
    return exchange(jnp.broadcast_to(shard[None], (lax.axis_size(axis), *shard.shape)), axis)


def rotate(values, places):
    half = values.shape[-1] // 2
    freq = 10000.0 ** (-(jnp.arange(half, dtype=jnp.float32) * 2.0 / values.shape[-1]))
    angle = places[..., None, None] * freq
    first = values[..., :half]
    second = values[..., half:]
    cosine = jnp.cos(angle)
    sine = jnp.sin(angle)
    return jnp.concatenate(
        [first * cosine - second * sine, second * cosine + first * sine], axis=-1
    )


def gathered_blocks(block):
    blocks = block[None]
    zs = [0]
    for bit in (4, 2, 1):
        pairs = [(i, i ^ bit) for i in range(lax.axis_size("z"))]
        blocks = jnp.concatenate([blocks, lax.ppermute(blocks, "z", pairs)], axis=0)
        zs = zs + [m ^ bit for m in zs]
    other = lax.ppermute(blocks, "core", [(0, 1), (1, 0)])
    return blocks, other, zs


def on_device(
    actions,
    lengths,
    embed,
    attn_gain,
    w_query,
    w_key,
    w_value,
    w_out,
    key_cache,
    value_cache,
    final_gain,
    head,
):
    s = lax.axis_index(SEQ)
    g = lax.axis_index(GRP)
    seqs = lax.axis_size(SEQ)
    groups = lax.axis_size(GRP)
    robots, steps = actions.shape
    rows = robots * steps
    prompt_dev, width = key_cache.shape[1:]
    cols = w_query.shape[1]
    feats = w_query.shape[0]
    bins = embed.shape[0]
    own_bins = head.shape[0]
    lh = cols // HEAD_DIM
    scale = HEAD_DIM ** (-0.5)
    bin_ids = jnp.arange(bins, dtype=jnp.int32)

    w_mine, w_other, zs = gathered_blocks(w_out)

    acts = copy_for_each(actions.reshape(rows), GRP).reshape(groups * rows)
    wide = embed.astype(jnp.float32)
    mean_square = jnp.mean(wide * wide, axis=-1, keepdims=True)
    part = lax.dynamic_slice(embed, (0, g * feats), (bins, feats)).astype(jnp.float32)
    part_gain = lax.dynamic_slice(attn_gain, (g * feats,), (feats,))
    table = (part * lax.rsqrt(mean_square + 1e-05) * part_gain).astype(jnp.bfloat16)
    onehot = (acts[:, None] == bin_ids[None, :]).astype(jnp.bfloat16)
    normed = jnp.dot(onehot, table, preferred_element_type=jnp.float32).astype(jnp.bfloat16)
    weights = jnp.concatenate([w_query, w_key, w_value], axis=1)
    terms = jnp.dot(normed, weights, preferred_element_type=jnp.float32).astype(jnp.bfloat16)
    sums = exchange(terms.reshape(groups, rows, 3 * cols), GRP)
    sums = jnp.sum(sums.astype(jnp.float32), axis=0)

    places = (lengths[:, None] + jnp.arange(steps, dtype=jnp.int32)[None, :]).astype(jnp.float32)
    heads_of = lambda flat: flat.reshape(robots, steps, lh, HEAD_DIM)
    query = rotate(heads_of(sums[:, :cols]), places).astype(jnp.bfloat16)
    key = rotate(heads_of(sums[:, cols : 2 * cols]), places).astype(jnp.bfloat16)
    value = heads_of(sums[:, 2 * cols :]).astype(jnp.bfloat16)

    head_parts = jnp.swapaxes(head.reshape(own_bins, seqs, cols), 0, 1)
    flat_query = jnp.broadcast_to(query.reshape(1, rows, cols), (seqs, rows, cols))
    spread = exchange(jnp.concatenate([flat_query, head_parts], axis=1), SEQ)
    all_query = spread[:, :rows].reshape(seqs, robots, steps, lh, HEAD_DIM)
    head_cols = spread[:, rows:].reshape(bins, cols)

    prompt_ids = s * prompt_dev + jnp.arange(prompt_dev, dtype=jnp.int32)
    mask = (prompt_ids[None, :] < lengths[:, None])[:, None, None, :]
    heads = seqs * lh
    q = jnp.moveaxis(all_query, 0, 2).reshape(robots, steps, heads, HEAD_DIM)
    cache_keys = key_cache.reshape(robots, prompt_dev, heads, HEAD_DIM)
    cache_values = value_cache.reshape(robots, prompt_dev, heads, HEAD_DIM)
    scores = jnp.einsum("rthd,rphd->rhtp", q, cache_keys, preferred_element_type=jnp.float32)
    scores = jnp.where(mask, scores * scale, NEG)
    top = jnp.max(scores, axis=-1)
    e = jnp.where(mask, jnp.exp(scores - top[..., None]), 0.0)
    total = jnp.sum(e, axis=-1)
    acc = jnp.einsum(
        "rhtp,rphd->rhtd", e.astype(jnp.bfloat16), cache_values, preferred_element_type=jnp.float32
    )

    def to_owner(x):
        x = x.reshape(robots, seqs, lh, steps, -1)
        return jnp.moveaxis(x, 1, 0).reshape(seqs, robots * lh * steps, -1)

    stats = jnp.concatenate([to_owner(top)[..., 0], to_owner(total)[..., 0]], axis=-1)
    stats = jnp.pad(stats, ((0, 0), (0, -stats.shape[-1] % HEAD_DIM))).reshape(seqs, -1, HEAD_DIM)
    packed = exchange(jnp.concatenate([to_owner(acc), stats], axis=1), SEQ)
    n = robots * lh * steps
    tops = packed[:, n:].reshape(seqs, -1)[:, :n]
    totals = packed[:, n:].reshape(seqs, -1)[:, n : 2 * n]
    accs = packed[:, :n]

    step_ids = jnp.arange(steps, dtype=jnp.int32)
    causal = step_ids[None, :] <= step_ids[:, None]
    w_scores = jnp.einsum("rthd,rjhd->rhtj", query, key, preferred_element_type=jnp.float32)
    w_scores = jnp.where(causal, w_scores * scale, NEG)
    w_top = jnp.max(w_scores, axis=-1)
    w_e = jnp.where(causal, jnp.exp(w_scores - w_top[..., None]), 0.0)
    w_total = jnp.sum(w_e, axis=-1).reshape(n)
    w_acc = jnp.einsum(
        "rhtj,rjhd->rhtd", w_e.astype(jnp.bfloat16), value, preferred_element_type=jnp.float32
    ).reshape(n, HEAD_DIM)
    w_top = w_top.reshape(n)

    best = jnp.maximum(jnp.max(tops, axis=0), w_top)
    factors = jnp.exp(tops - best[None])
    w_factor = jnp.exp(w_top - best)
    denom = jnp.sum(totals * factors, axis=0) + w_total * w_factor
    numer = jnp.sum(accs * factors[..., None], axis=0) + w_acc * w_factor[:, None]
    attended = (numer / denom[:, None]).astype(jnp.bfloat16)
    attended = attended.reshape(robots, lh, steps, HEAD_DIM).swapaxes(1, 2).reshape(rows, cols)

    blocks = copy_for_each(attended, SEQ)
    z = lax.axis_index("z")
    core = lax.axis_index("core")
    zc = lax.axis_size("core")
    order = (z ^ jnp.array(zs, jnp.int32)) * zc
    mine = jnp.moveaxis(jnp.take(blocks, order + core, axis=0), 0, 1).reshape(rows, -1)
    others = jnp.moveaxis(jnp.take(blocks, order + 1 - core, axis=0), 0, 1).reshape(rows, -1)
    branch = jnp.dot(mine, w_mine.reshape(-1, cols), preferred_element_type=jnp.float32)
    branch += jnp.dot(others, w_other.reshape(-1, cols), preferred_element_type=jnp.float32)

    own_hot = (actions.reshape(rows)[:, None] == bin_ids[None, :]).astype(jnp.bfloat16)
    own_embed = lax.dynamic_slice(embed, (0, s * cols), (bins, cols))
    inputs = jnp.dot(own_hot, own_embed, preferred_element_type=jnp.float32)
    residual = inputs + branch
    gained = (residual * lax.dynamic_slice(final_gain, (s * cols,), (cols,))).astype(jnp.bfloat16)
    part_logits = lax.dot_general(
        gained, head_cols, (((1,), (1,)), ((), ())), preferred_element_type=jnp.float32
    )
    squares = jnp.sum(residual * residual, axis=-1)
    squares = jnp.pad(squares, (0, bins - rows))[None]
    parts = jnp.concatenate([part_logits, squares, jnp.zeros((1, bins), jnp.float32)], axis=0)
    summed = jnp.sum(copy_for_each(parts, SEQ), axis=0)
    inverse = lax.rsqrt(summed[rows, :rows] / width + 1e-05)
    logits = summed[:rows] * inverse[:, None]
    top_logit = jnp.max(logits, axis=-1, keepdims=True)
    exp_total = jnp.sum(jnp.exp(logits - top_logit), axis=-1, keepdims=True)
    own = lax.dynamic_slice(logits, (0, s * own_bins), (rows, own_bins))
    logprob = own - top_logit - jnp.log(exp_total)
    return logprob.reshape(robots, steps, own_bins)


def solution(mesh):
    torus = Mesh(mesh.devices.reshape(4, 4, 8, 2), ("seq_0", "seq_1", "z", "core"))
    in_specs = (
        P(GRP, None),
        P(GRP),
        P(),
        P(),
        P(GRP, SEQ),
        P(GRP, SEQ),
        P(GRP, SEQ),
        P(GRP, SEQ),
        P(GRP, SEQ, None),
        P(GRP, SEQ, None),
        P(),
        P(SEQ, None),
    )
    out_specs = P(GRP, None, SEQ)
    return jax.shard_map(
        on_device, mesh=torus, in_specs=in_specs, out_specs=out_specs, check_vma=False
    )
```

```python
import jax
import jax.numpy as jnp
from jax import lax
from jax.sharding import Mesh
from jax.sharding import PartitionSpec as P


HEAD_DIM = 128
SEQ = ("seq_0", "seq_1")
GRP = ("z", "core")
NEG = -1e30


def exchange(pieces, axis):
    return lax.all_to_all(pieces, axis, split_axis=0, concat_axis=0, tiled=True)


def copy_for_each(shard, axis):
    return exchange(jnp.broadcast_to(shard[None], (lax.axis_size(axis), *shard.shape)), axis)


def from_partner(x, axis, k):
    return lax.ppermute(x, axis, [(i, i ^ k) for i in range(lax.axis_size(axis))])


def in_order(own, axis):
    i = lax.axis_index(axis)
    odd = (i & 1) == 1
    high = (i & 2) == 2
    a, b, c, d = own
    a, b = jnp.where(odd, b, a), jnp.where(odd, a, b)
    c, d = jnp.where(odd, d, c), jnp.where(odd, c, d)
    return (
        jnp.where(high, c, a),
        jnp.where(high, d, b),
        jnp.where(high, a, c),
        jnp.where(high, b, d),
    )


def from_all(x, axis):
    return (x, *(from_partner(x, axis, k) for k in (1, 2, 3)))


def after(x, anchor):
    return lax.optimization_barrier((x, anchor))[0]


def halves(x):
    both = lax.reduce_precision(x, 8, 15)
    high = lax.reduce_precision(both, 8, 7)
    return high.astype(jnp.bfloat16), (both - high).astype(jnp.bfloat16), both


def joined(high, low):
    return high.astype(jnp.float32) + low.astype(jnp.float32)


def merge(tops, totals, accs):
    best = tops[0]
    for t in tops[1:]:
        best = jnp.maximum(best, t)
    factors = [jnp.exp(t - best) for t in tops]
    total = sum(l * f for l, f in zip(totals, factors))
    acc = sum(x.astype(jnp.float32) * f[:, None] for x, f in zip(accs, factors))
    return best, total, acc


def packed(top, total, acc):
    th, tl, _ = halves(top)
    lh, ll, _ = halves(total)
    stats = jnp.stack([th, tl, lh, ll])
    stats = jnp.pad(stats, ((0, 12), (0, 0)))
    return jnp.concatenate([acc.astype(jnp.bfloat16), stats], axis=0)


def unpacked(x):
    n = x.shape[1]
    stats = x[n : n + 4]
    return joined(stats[0], stats[1]), joined(stats[2], stats[3]), x[:n]


def rotate(values, places):
    half = values.shape[-1] // 2
    freq = 10000.0 ** (-(jnp.arange(half, dtype=jnp.float32) * 2.0 / values.shape[-1]))
    angle = places[..., None, None] * freq
    first = values[..., :half]
    second = values[..., half:]
    cosine = jnp.cos(angle)
    sine = jnp.sin(angle)
    return jnp.concatenate(
        [first * cosine - second * sine, second * cosine + first * sine], axis=-1
    )


def on_device(
    actions,
    lengths,
    embed,
    attn_gain,
    w_query,
    w_key,
    w_value,
    w_out,
    key_cache,
    value_cache,
    final_gain,
    head,
):
    s0 = lax.axis_index("seq_0")
    s = lax.axis_index(SEQ)
    g = lax.axis_index(GRP)
    z = lax.axis_index("z")
    core = lax.axis_index("core")
    seqs = lax.axis_size(SEQ)
    side = lax.axis_size("seq_0")
    groups = lax.axis_size(GRP)
    robots, true_steps = actions.shape
    steps = 8
    rows = robots * steps
    prompt_dev, width = key_cache.shape[1:]
    feats, cols = w_query.shape
    bins = embed.shape[0]
    own_bins = head.shape[0]
    lh = cols // HEAD_DIM
    heads = seqs * lh
    scale = HEAD_DIM ** (-0.5)
    bin_ids = jnp.arange(bins, dtype=jnp.int32)

    blocks = w_out[None]
    zs = [0]
    blocks = jnp.concatenate([blocks, from_partner(blocks, "z", 4)], axis=0)
    zs = zs + [m ^ 4 for m in zs]

    pad_steps = ((0, 0), (0, steps - true_steps))
    acts = copy_for_each(actions, GRP).reshape(groups * robots, true_steps)
    acts = jnp.pad(acts, pad_steps).reshape(groups * rows)
    actions = jnp.pad(actions, pad_steps)
    wide = embed.astype(jnp.float32)
    mean_square = jnp.mean(wide * wide, axis=-1, keepdims=True)
    part = lax.dynamic_slice(embed, (0, g * feats), (bins, feats)).astype(jnp.float32)
    part_gain = lax.dynamic_slice(attn_gain, (g * feats,), (feats,))
    table = (part * lax.rsqrt(mean_square + 1e-05) * part_gain).astype(jnp.bfloat16)
    onehot = (acts[:, None] == bin_ids[None, :]).astype(jnp.bfloat16)
    normed = jnp.dot(onehot, table, preferred_element_type=jnp.float32).astype(jnp.bfloat16)
    weights = jnp.concatenate([w_query, w_key, w_value], axis=1)
    terms = jnp.dot(normed, weights, preferred_element_type=jnp.float32).astype(jnp.bfloat16)
    sums = exchange(terms.reshape(groups, rows, 3 * cols), GRP)
    sums = jnp.sum(sums.astype(jnp.float32), axis=0)

    blocks = after(blocks, sums)
    blocks = jnp.concatenate([blocks, from_partner(blocks, "z", 2)], axis=0)
    zs = zs + [m ^ 2 for m in zs]

    places = (lengths[:, None] + jnp.arange(steps, dtype=jnp.int32)[None, :]).astype(jnp.float32)
    heads_of = lambda flat: flat.reshape(robots, steps, lh, HEAD_DIM)
    query = rotate(heads_of(sums[:, :cols]), places).astype(jnp.bfloat16)
    key = rotate(heads_of(sums[:, cols : 2 * cols]), places).astype(jnp.bfloat16)
    value = heads_of(sums[:, 2 * cols :]).astype(jnp.bfloat16)

    flat_query = query.reshape(1, rows, cols)
    head_parts = head.reshape(own_bins, side, side, cols).transpose(2, 1, 0, 3)
    head_parts = in_order([head_parts[k] for k in range(side)], "seq_1")
    near = [jnp.concatenate([flat_query, head_parts[0]], axis=0)]
    for k in (1, 2, 3):
        sent = jnp.concatenate([flat_query, head_parts[k]], axis=0)
        near.append(from_partner(sent, "seq_1", k))
    near = jnp.stack(in_order(near, "seq_1"))
    head_parts = in_order([near[:, 1 + k] for k in range(side)], "seq_0")
    far = [jnp.concatenate([near[:, 0], head_parts[0]], axis=0)]
    for k in (1, 2, 3):
        sent = jnp.concatenate([near[:, 0], head_parts[k]], axis=0)
        far.append(from_partner(sent, "seq_0", k))
    far = jnp.stack(in_order(far, "seq_0"))
    all_query = far[:, :side].reshape(seqs, robots, steps, lh, HEAD_DIM)
    head_cols = far[:, side:].reshape(bins, cols)

    prompt_ids = s * prompt_dev + jnp.arange(prompt_dev, dtype=jnp.int32)
    mask = (prompt_ids[None, :] < lengths[:, None])[:, None, None, :]
    q = jnp.moveaxis(all_query, 0, 2).reshape(robots, steps, heads, HEAD_DIM)
    cache_keys = key_cache.reshape(robots, prompt_dev, heads, HEAD_DIM)
    cache_values = value_cache.reshape(robots, prompt_dev, heads, HEAD_DIM)
    scores = jnp.einsum("rthd,rphd->rhtp", q, cache_keys, preferred_element_type=jnp.float32)
    scores = jnp.where(mask, scores * scale, NEG)
    top = lax.reduce_precision(jnp.max(scores, axis=-1), 8, 15)
    e = jnp.where(mask, jnp.exp(scores - top[..., None]), 0.0)
    total = jnp.sum(e, axis=-1)
    acc = jnp.einsum(
        "rhtp,rphd->rhtd", e.astype(jnp.bfloat16), cache_values, preferred_element_type=jnp.float32
    )
    blocks = after(blocks, acc)
    blocks = jnp.concatenate([blocks, from_partner(blocks, "z", 1)], axis=0)
    zs = zs + [m ^ 1 for m in zs]

    step_ids = jnp.arange(steps, dtype=jnp.int32)
    causal = step_ids[None, :] <= step_ids[:, None]
    w_scores = jnp.einsum("rthd,rjhd->rhtj", query, key, preferred_element_type=jnp.float32)
    w_scores = jnp.where(causal, w_scores * scale, NEG)
    w_top = lax.reduce_precision(jnp.max(w_scores, axis=-1), 8, 15)
    w_e = jnp.where(causal, jnp.exp(w_scores - w_top[..., None]), 0.0)
    w_total = jnp.sum(w_e, axis=-1)
    w_acc = jnp.einsum(
        "rhtj,rjhd->rhtd", w_e.astype(jnp.bfloat16), value, preferred_element_type=jnp.float32
    )

    def quarters(x):
        x = x.reshape(robots, side, side, lh, steps, -1)
        return [x[:, k].reshape(robots * side * lh * steps, -1) for k in range(side)]

    tops = in_order(quarters(top), "seq_0")
    totals = in_order(quarters(total), "seq_0")
    accs = in_order(quarters(acc.astype(jnp.bfloat16)), "seq_0")
    pieces = [(tops[0][:, 0], totals[0][:, 0], accs[0])]
    for k in (1, 2, 3):
        sent = packed(tops[k][:, 0], totals[k][:, 0], accs[k])
        pieces.append(unpacked(from_partner(sent, "seq_0", k)))
    top, total, acc = merge(*zip(*pieces))

    s1 = lax.axis_index("seq_1")
    at_owner = (jnp.arange(side) == s1)[None, :, None, None]
    spread = lambda x: jnp.broadcast_to(x[:, None], (robots, side, *x.shape[1:]))
    flat = lambda x: x.reshape(robots * side * lh * steps, *x.shape[4:])
    w_top = flat(jnp.where(at_owner, spread(w_top), NEG))
    w_total = flat(jnp.where(at_owner, spread(w_total), 0.0))
    w_acc = flat(jnp.where(at_owner[..., None], spread(w_acc), 0.0))
    top, total, acc = merge((top, w_top), (total, w_total), (acc, w_acc))

    sent = packed(top, total, acc)
    _, _, total = halves(total)
    pieces = [(top, total, sent[: acc.shape[0]])]
    for k in (1, 2, 3):
        pieces.append(unpacked(from_partner(sent, "seq_1", k)))
    top, total, acc = merge(*zip(*pieces))
    attended = (acc / total[:, None]).astype(jnp.bfloat16)
    attended = attended.reshape(robots, side, lh, steps, HEAD_DIM)
    attended = attended.transpose(1, 0, 3, 2, 4).reshape(side, rows, cols)

    blocks = after(blocks, attended)
    other = from_partner(blocks, "core", 1)

    gathered = jnp.concatenate(from_all(attended, "seq_0"), axis=0)
    order = (z ^ jnp.array(zs, jnp.int32)) * lax.axis_size("core")
    place = lambda b: ((b // side) ^ s0) * side + b % side
    take = lambda b: jnp.moveaxis(jnp.take(gathered, place(b), axis=0), 0, 1).reshape(rows, -1)
    branch = jnp.dot(take(order + core), blocks.reshape(-1, cols), preferred_element_type=jnp.float32)
    branch += jnp.dot(take(order + 1 - core), other.reshape(-1, cols), preferred_element_type=jnp.float32)

    own_hot = (actions.reshape(rows)[:, None] == bin_ids[None, :]).astype(jnp.bfloat16)
    own_embed = lax.dynamic_slice(embed, (0, s * cols), (bins, cols))
    inputs = jnp.dot(own_hot, own_embed, preferred_element_type=jnp.float32)
    residual = inputs + branch
    gained = (residual * lax.dynamic_slice(final_gain, (s * cols,), (cols,))).astype(jnp.bfloat16)
    part_logits = lax.dot_general(
        gained, head_cols, (((1,), (1,)), ((), ())), preferred_element_type=jnp.float32
    )
    squares = jnp.sum(residual * residual, axis=-1)
    last = (jnp.arange(rows) == rows - 1)[:, None]
    parts = jnp.where(last, jnp.pad(squares, (0, bins - rows))[None], part_logits)
    parts = sum(from_all(parts, "seq_1"))
    parts = sum(from_all(parts, "seq_0"))
    inverse = lax.rsqrt(parts[rows - 1, :rows] / width + 1e-05)
    logits = parts * inverse[:, None]
    top_logit = jnp.max(logits, axis=-1, keepdims=True)
    exp_total = jnp.sum(jnp.exp(logits - top_logit), axis=-1, keepdims=True)
    own = lax.dynamic_slice(parts, (0, s * own_bins), (rows, own_bins)) * inverse[:, None]
    logprob = own - top_logit - jnp.log(exp_total)
    return logprob.reshape(robots, steps, own_bins)[:, :true_steps]


def solution(mesh):
    torus = Mesh(mesh.devices.reshape(4, 4, 8, 2), ("seq_0", "seq_1", "z", "core"))
    in_specs = (
        P(GRP, None),
        P(GRP),
        P(),
        P(),
        P(GRP, SEQ),
        P(GRP, SEQ),
        P(GRP, SEQ),
        P(GRP, SEQ),
        P(GRP, SEQ, None),
        P(GRP, SEQ, None),
        P(),
        P(SEQ, None),
    )
    out_specs = P(GRP, None, SEQ)

    return jax.shard_map(
        on_device, mesh=torus, in_specs=in_specs, out_specs=out_specs, check_vma=False
    )
```

```python
import jax
import jax.numpy as jnp
from jax import lax
from jax.sharding import Mesh
from jax.sharding import PartitionSpec as P


HEAD_DIM = 128
SEQ = ("seq_0", "seq_1")
GRP = ("z", "core")
NEG = -1e30


def exchange(pieces, axis):
    return lax.all_to_all(pieces, axis, split_axis=0, concat_axis=0, tiled=True)


def copy_for_each(shard, axis):
    return exchange(jnp.broadcast_to(shard[None], (lax.axis_size(axis), *shard.shape)), axis)


def from_partner(x, axis, k):
    return lax.ppermute(x, axis, [(i, i ^ k) for i in range(lax.axis_size(axis))])


def in_order(own, axis):
    i = lax.axis_index(axis)
    odd = (i & 1) == 1
    high = (i & 2) == 2
    a, b, c, d = own
    a, b = jnp.where(odd, b, a), jnp.where(odd, a, b)
    c, d = jnp.where(odd, d, c), jnp.where(odd, c, d)
    return (
        jnp.where(high, c, a),
        jnp.where(high, d, b),
        jnp.where(high, a, c),
        jnp.where(high, b, d),
    )


def from_all(x, axis):
    return (x, *(from_partner(x, axis, k) for k in (1, 2, 3)))


def after(x, anchor):
    return lax.optimization_barrier((x, anchor))[0]


def halves(x):
    both = lax.reduce_precision(x, 8, 15)
    high = lax.reduce_precision(both, 8, 7)
    return high.astype(jnp.bfloat16), (both - high).astype(jnp.bfloat16), both


def joined(high, low):
    return high.astype(jnp.float32) + low.astype(jnp.float32)


def merge(tops, totals, accs):
    best = tops[0]
    for t in tops[1:]:
        best = jnp.maximum(best, t)
    factors = [jnp.exp(t - best) for t in tops]
    total = sum(l * f for l, f in zip(totals, factors))
    acc = sum(x.astype(jnp.float32) * f[:, None] for x, f in zip(accs, factors))
    return best, total, acc


def packed(top, total, acc):
    th, tl, _ = halves(top)
    lh, ll, _ = halves(total)
    stats = jnp.stack([th, tl, lh, ll])
    stats = jnp.pad(stats, ((0, 12), (0, 0)))
    return jnp.concatenate([acc.astype(jnp.bfloat16), stats], axis=0)


def unpacked(x):
    n = x.shape[1]
    stats = x[n : n + 4]
    return joined(stats[0], stats[1]), joined(stats[2], stats[3]), x[:n]


def rotate(values, places):
    half = values.shape[-1] // 2
    freq = 10000.0 ** (-(jnp.arange(half, dtype=jnp.float32) * 2.0 / values.shape[-1]))
    angle = places[..., None, None] * freq
    first = values[..., :half]
    second = values[..., half:]
    cosine = jnp.cos(angle)
    sine = jnp.sin(angle)
    return jnp.concatenate(
        [first * cosine - second * sine, second * cosine + first * sine], axis=-1
    )


def on_device(
    actions,
    lengths,
    embed,
    attn_gain,
    w_query,
    w_key,
    w_value,
    w_out,
    key_cache,
    value_cache,
    final_gain,
    head,
):
    s0 = lax.axis_index("seq_0")
    s = lax.axis_index(SEQ)
    g = lax.axis_index(GRP)
    z = lax.axis_index("z")
    core = lax.axis_index("core")
    seqs = lax.axis_size(SEQ)
    side = lax.axis_size("seq_0")
    groups = lax.axis_size(GRP)
    robots, true_steps = actions.shape
    steps = 8
    rows = robots * steps
    prompt_dev, width = key_cache.shape[1:]
    feats, cols = w_query.shape
    bins = embed.shape[0]
    own_bins = head.shape[0]
    lh = cols // HEAD_DIM
    heads = seqs * lh
    scale = HEAD_DIM ** (-0.5)
    bin_ids = jnp.arange(bins, dtype=jnp.int32)

    blocks = w_out[None]
    zs = [0]
    blocks = jnp.concatenate([blocks, from_partner(blocks, "z", 4)], axis=0)
    zs = zs + [m ^ 4 for m in zs]

    pad_steps = ((0, 0), (0, steps - true_steps))
    acts = copy_for_each(actions, GRP).reshape(groups * robots, true_steps)
    acts = jnp.pad(acts, pad_steps).reshape(groups * rows)
    actions = jnp.pad(actions, pad_steps)
    wide = embed.astype(jnp.float32)
    mean_square = jnp.mean(wide * wide, axis=-1, keepdims=True)
    part = lax.dynamic_slice(embed, (0, g * feats), (bins, feats)).astype(jnp.float32)
    part_gain = lax.dynamic_slice(attn_gain, (g * feats,), (feats,))
    table = (part * lax.rsqrt(mean_square + 1e-05) * part_gain).astype(jnp.bfloat16)
    onehot = (acts[:, None] == bin_ids[None, :]).astype(jnp.bfloat16)
    normed = jnp.dot(onehot, table, preferred_element_type=jnp.float32).astype(jnp.bfloat16)
    weights = jnp.concatenate([w_query, w_key, w_value], axis=1)
    terms = jnp.dot(normed, weights, preferred_element_type=jnp.float32).astype(jnp.bfloat16)
    sums = exchange(terms.reshape(groups, rows, 3 * cols), GRP)
    sums = jnp.sum(sums.astype(jnp.float32), axis=0)

    head = after(head, terms).reshape(own_bins, side, side, cols).transpose(2, 1, 0, 3)
    head = in_order([head[k] for k in range(side)], "seq_1")
    head = (head[0], *(from_partner(head[k], "seq_1", k) for k in (1, 2, 3)))
    head = jnp.stack(in_order(head, "seq_1"), axis=1)
    head = in_order([head[k] for k in range(side)], "seq_0")
    head = (head[0], *(from_partner(head[k], "seq_0", k) for k in (1, 2, 3)))
    head_cols = jnp.stack(in_order(head, "seq_0")).reshape(bins, cols)
    own_hot = (after(actions, terms).reshape(rows)[:, None] == bin_ids[None, :]).astype(jnp.bfloat16)
    own_embed = lax.dynamic_slice(embed, (0, s * cols), (bins, cols))
    inputs = jnp.dot(own_hot, own_embed, preferred_element_type=jnp.float32)
    own_gain = lax.dynamic_slice(after(final_gain, terms), (s * cols,), (cols,))
    lengths = after(lengths, terms)

    blocks = after(blocks, sums)
    blocks = jnp.concatenate([blocks, from_partner(blocks, "z", 2)], axis=0)
    zs = zs + [m ^ 2 for m in zs]

    (sums, head_cols, inputs, own_gain, lengths) = lax.optimization_barrier(
        (sums, head_cols, inputs, own_gain, lengths)
    )
    places = (lengths[:, None] + jnp.arange(steps, dtype=jnp.int32)[None, :]).astype(jnp.float32)
    heads_of = lambda flat: flat.reshape(robots, steps, lh, HEAD_DIM)
    query = rotate(heads_of(sums[:, :cols]), places).astype(jnp.bfloat16)
    key = rotate(heads_of(sums[:, cols : 2 * cols]), places).astype(jnp.bfloat16)
    value = heads_of(sums[:, 2 * cols :]).astype(jnp.bfloat16)

    flat_query = query.reshape(rows, cols)
    near = jnp.stack(in_order(from_all(flat_query, "seq_1"), "seq_1"))
    far = jnp.stack(in_order(from_all(near, "seq_0"), "seq_0"))
    all_query = far.reshape(seqs, robots, steps, lh, HEAD_DIM)

    prompt_ids = s * prompt_dev + jnp.arange(prompt_dev, dtype=jnp.int32)
    mask = (prompt_ids[None, :] < lengths[:, None])[:, None, None, :]
    q = jnp.moveaxis(all_query, 0, 2).reshape(robots, steps, heads, HEAD_DIM)
    cache_keys = key_cache.reshape(robots, prompt_dev, heads, HEAD_DIM)
    cache_values = value_cache.reshape(robots, prompt_dev, heads, HEAD_DIM)
    scores = jnp.einsum("rthd,rphd->rhtp", q, cache_keys, preferred_element_type=jnp.float32)
    scores = jnp.where(mask, scores * scale, NEG)
    top = lax.reduce_precision(jnp.max(scores, axis=-1), 8, 15)
    e = jnp.where(mask, jnp.exp(scores - top[..., None]), 0.0)
    total = jnp.sum(e, axis=-1)
    acc = jnp.einsum(
        "rhtp,rphd->rhtd", e.astype(jnp.bfloat16), cache_values, preferred_element_type=jnp.float32
    )
    blocks = after(blocks, acc)
    blocks = jnp.concatenate([blocks, from_partner(blocks, "z", 1)], axis=0)
    zs = zs + [m ^ 1 for m in zs]

    step_ids = jnp.arange(steps, dtype=jnp.int32)
    causal = step_ids[None, :] <= step_ids[:, None]
    w_scores = jnp.einsum("rthd,rjhd->rhtj", query, key, preferred_element_type=jnp.float32)
    w_scores = jnp.where(causal, w_scores * scale, NEG)
    w_top = lax.reduce_precision(jnp.max(w_scores, axis=-1), 8, 15)
    w_e = jnp.where(causal, jnp.exp(w_scores - w_top[..., None]), 0.0)
    w_total = jnp.sum(w_e, axis=-1)
    w_acc = jnp.einsum(
        "rhtj,rjhd->rhtd", w_e.astype(jnp.bfloat16), value, preferred_element_type=jnp.float32
    )

    def quarters(x):
        x = x.reshape(robots, side, side, lh, steps, -1)
        return [x[:, k].reshape(robots * side * lh * steps, -1) for k in range(side)]

    tops = in_order(quarters(top), "seq_0")
    totals = in_order(quarters(total), "seq_0")
    accs = in_order(quarters(acc.astype(jnp.bfloat16)), "seq_0")
    pieces = [(tops[0][:, 0], totals[0][:, 0], accs[0])]
    for k in (1, 2, 3):
        sent = packed(tops[k][:, 0], totals[k][:, 0], accs[k])
        pieces.append(unpacked(from_partner(sent, "seq_0", k)))
    top, total, acc = merge(*zip(*pieces))

    s1 = lax.axis_index("seq_1")
    at_owner = (jnp.arange(side) == s1)[None, :, None, None]
    spread = lambda x: jnp.broadcast_to(x[:, None], (robots, side, *x.shape[1:]))
    flat = lambda x: x.reshape(robots * side * lh * steps, *x.shape[4:])
    w_top = flat(jnp.where(at_owner, spread(w_top), NEG))
    w_total = flat(jnp.where(at_owner, spread(w_total), 0.0))
    w_acc = flat(jnp.where(at_owner[..., None], spread(w_acc), 0.0))
    top, total, acc = merge((top, w_top), (total, w_total), (acc, w_acc))

    sent = packed(top, total, acc)
    _, _, total = halves(total)
    pieces = [(top, total, sent[: acc.shape[0]])]
    for k in (1, 2, 3):
        pieces.append(unpacked(from_partner(sent, "seq_1", k)))
    top, total, acc = merge(*zip(*pieces))
    attended = (acc / total[:, None]).astype(jnp.bfloat16)
    attended = attended.reshape(robots, side, lh, steps, HEAD_DIM)
    attended = attended.transpose(1, 0, 3, 2, 4).reshape(side, rows, cols)

    blocks = after(blocks, attended)
    other = from_partner(blocks, "core", 1)

    gathered = jnp.concatenate(from_all(attended, "seq_0"), axis=0)
    order = (z ^ jnp.array(zs, jnp.int32)) * lax.axis_size("core")
    place = lambda b: ((b // side) ^ s0) * side + b % side
    take = lambda b: jnp.moveaxis(jnp.take(gathered, place(b), axis=0), 0, 1).reshape(rows, -1)
    branch = jnp.dot(take(order + core), blocks.reshape(-1, cols), preferred_element_type=jnp.float32)
    branch += jnp.dot(take(order + 1 - core), other.reshape(-1, cols), preferred_element_type=jnp.float32)

    residual = inputs + branch
    gained = (residual * own_gain).astype(jnp.bfloat16)
    part_logits = lax.dot_general(
        gained, head_cols, (((1,), (1,)), ((), ())), preferred_element_type=jnp.float32
    )
    squares = jnp.sum(residual * residual, axis=-1)
    last = (jnp.arange(rows) == rows - 1)[:, None]
    parts = jnp.where(last, jnp.pad(squares, (0, bins - rows))[None], part_logits)
    parts = sum(from_all(parts, "seq_1"))
    parts = sum(from_all(parts, "seq_0"))
    inverse = lax.rsqrt(parts[rows - 1, :rows] / width + 1e-05)
    logits = parts * inverse[:, None]
    top_logit = jnp.max(logits, axis=-1, keepdims=True)
    exp_total = jnp.sum(jnp.exp(logits - top_logit), axis=-1, keepdims=True)
    own = lax.dynamic_slice(parts, (0, s * own_bins), (rows, own_bins)) * inverse[:, None]
    logprob = own - top_logit - jnp.log(exp_total)
    return logprob.reshape(robots, steps, own_bins)[:, :true_steps]


def solution(mesh):
    torus = Mesh(mesh.devices.reshape(4, 4, 8, 2), ("seq_0", "seq_1", "z", "core"))
    in_specs = (
        P(GRP, None),
        P(GRP),
        P(),
        P(),
        P(GRP, SEQ),
        P(GRP, SEQ),
        P(GRP, SEQ),
        P(GRP, SEQ),
        P(GRP, SEQ, None),
        P(GRP, SEQ, None),
        P(),
        P(SEQ, None),
    )
    out_specs = P(GRP, None, SEQ)

    return jax.shard_map(
        on_device, mesh=torus, in_specs=in_specs, out_specs=out_specs, check_vma=False
    )
```

```python
import functools

import jax
import jax.numpy as jnp
from jax import lax
from jax.experimental import pallas as pl
from jax.experimental.pallas import tpu as pltpu
from jax.sharding import Mesh
from jax.sharding import PartitionSpec as P


HEAD_DIM = 128
SEQ = ("seq_0", "seq_1")
GRP = ("z", "core")
NEG = -1e30


def exchange(pieces, axis):
    return lax.all_to_all(pieces, axis, split_axis=0, concat_axis=0, tiled=True)


def from_partner(x, axis, k):
    return lax.ppermute(x, axis, [(i, i ^ k) for i in range(lax.axis_size(axis))])


def fenced(*arrays):
    return lax.optimization_barrier(arrays)


def halves(x):
    both = lax.reduce_precision(x, 8, 15)
    high = lax.reduce_precision(both, 8, 7)
    return high.astype(jnp.bfloat16), (both - high).astype(jnp.bfloat16), both


def in_vmem():
    return pl.BlockSpec(memory_space=pltpu.VMEM)


def in_smem():
    return pl.BlockSpec(memory_space=pltpu.SMEM)


def call(kernel, out, specs, *args):
    outs = (in_vmem(),) * len(out) if isinstance(out, tuple) else in_vmem()
    small = pltpu.CompilerParams(vmem_limit_bytes=8 * 2**20)
    return pl.pallas_call(
        kernel, out_shape=out, in_specs=specs, out_specs=outs, compiler_params=small
    )(*args)


def merge_kernel(query, key, value, stats, packed, out):
    seqs, _, head_dim = packed.shape
    rows, cols = query.shape
    lh = cols // head_dim
    steps = 8
    n = rows * lh
    scale = head_dim ** (-0.5)
    causal = lax.broadcasted_iota(jnp.int32, (steps, steps), 1) <= lax.broadcasted_iota(
        jnp.int32, (steps, steps), 0
    )
    tops, totals, accs = [], [], []
    for r in range(rows // steps):
        for h in range(lh):
            at = (slice(r * steps, (r + 1) * steps), slice(h * head_dim, (h + 1) * head_dim))
            q, k, v = (ref[at].astype(jnp.bfloat16) for ref in (query, key, value))
            scores = lax.dot_general(
                q, k, (((1,), (1,)), ((), ())), preferred_element_type=jnp.float32
            )
            scores = jnp.where(causal, scores * scale, NEG)
            top = jnp.max(scores, axis=-1, keepdims=True)
            e = jnp.where(causal, jnp.exp(scores - top), 0.0)
            tops.append(top)
            totals.append(jnp.sum(e, axis=-1, keepdims=True))
            accs.append(jnp.dot(e.astype(jnp.bfloat16), v, preferred_element_type=jnp.float32))
    w_top, w_total, w_acc = (jnp.concatenate(x, axis=0) for x in (tops, totals, accs))
    part = stats[...].astype(jnp.float32)
    part = jnp.concatenate([part, jnp.zeros((4 * n - seqs, 4 * n), jnp.float32)], axis=0).T
    there = lax.broadcasted_iota(jnp.int32, (n, 4 * n), 1) < seqs
    top = jnp.where(there, part[:n] + part[n : 2 * n], NEG)
    total = part[2 * n : 3 * n] + part[3 * n :]
    best = jnp.maximum(jnp.max(top, axis=-1, keepdims=True), w_top)
    factor = jnp.where(there, jnp.exp(top - best), 0.0)
    w_factor = jnp.exp(w_top - best)
    denom = jnp.sum(total * factor, axis=-1, keepdims=True) + w_total * w_factor
    numer = w_acc * w_factor
    for d in range(seqs):
        numer += packed[d, :n, :].astype(jnp.float32) * factor[:, d : d + 1]
    attended = numer / denom
    lines = []
    for r in range(rows // steps):
        own = [attended[(r * lh + h) * steps : (r * lh + h + 1) * steps] for h in range(lh)]
        lines.append(jnp.concatenate(own, axis=1))
    attended = jnp.concatenate(lines, axis=0).astype(jnp.bfloat16)
    for d in range(seqs):
        out[d] = attended


def output_kernel(places, blocks, mine, other, inputs, gain, head, out):
    count = mine.shape[0]
    seqs, rows, _ = blocks.shape
    residual = inputs[...]
    for m in range(count):
        residual += jnp.dot(blocks[places[m]], mine[m], preferred_element_type=jnp.float32)
        residual += jnp.dot(blocks[places[count + m]], other[m], preferred_element_type=jnp.float32)
    gained = (residual * gain[...]).astype(jnp.bfloat16)
    logits = lax.dot_general(
        gained, head[...], (((1,), (1,)), ((), ())), preferred_element_type=jnp.float32
    )
    row = lax.broadcasted_iota(jnp.int32, logits.shape, 0)
    lane = lax.broadcasted_iota(jnp.int32, logits.shape, 1)
    squares = jnp.sum(residual * residual, axis=-1, keepdims=True)
    squares = jnp.sum(jnp.where(row == lane, squares, 0.0), axis=0, keepdims=True)
    result = jnp.where(row == rows - 1, squares, logits)
    for d in range(seqs):
        out[d] = result


def final_kernel(shard, parts, out, *, width, steps):
    seqs, rows, _ = parts.shape
    robots, true_steps, own_bins = out.shape
    total = parts[0]
    for d in range(1, seqs):
        total += parts[d]
    row = lax.broadcasted_iota(jnp.int32, total.shape, 0)
    lane = lax.broadcasted_iota(jnp.int32, total.shape, 1)
    squares = jnp.sum(
        jnp.where(row == lane, total[rows - 1 :], 0.0), axis=-1, keepdims=True
    )
    logits = total * lax.rsqrt(squares / width + 1e-05)
    top = jnp.max(logits, axis=-1, keepdims=True)
    logprob = logits - top - jnp.log(jnp.sum(jnp.exp(logits - top), axis=-1, keepdims=True))
    own = logprob[:, :own_bins]
    for k in range(1, seqs):
        own = jnp.where(shard[0] == k, logprob[:, k * own_bins : (k + 1) * own_bins], own)
    for r in range(robots):
        out[r] = own[r * steps : r * steps + true_steps]


def heads_kernel(sums, cosine, sine, head, spread, query, key, value):
    seqs = sums.shape[0]
    cols = query.shape[1]
    rows = query.shape[0]
    total = sums[0].astype(jnp.float32)
    for d in range(1, seqs):
        total += sums[d].astype(jnp.float32)

    def rotated(x):
        parts = []
        for h in range(cols // HEAD_DIM):
            part = x[:, h * HEAD_DIM : (h + 1) * HEAD_DIM]
            turned = pltpu.roll(part, HEAD_DIM // 2, 1)
            parts.append(part * cosine[...] + turned * sine[...])
        return jnp.concatenate(parts, axis=1)

    own = rotated(total[:, :cols])
    query[...] = own
    key[...] = rotated(total[:, cols : 2 * cols])
    value[...] = total[:, 2 * cols :]
    own = own.astype(jnp.bfloat16)
    for d in range(head.shape[0]):
        spread[d, :rows, :] = own
        spread[d, rows:, :] = head[d]


def on_device(
    actions,
    lengths,
    embed,
    attn_gain,
    w_query,
    w_key,
    w_value,
    w_out,
    key_cache,
    value_cache,
    final_gain,
    head,
):
    s = lax.axis_index(SEQ)
    g = lax.axis_index(GRP)
    z = lax.axis_index("z")
    core = lax.axis_index("core")
    seqs = lax.axis_size(SEQ)
    groups = lax.axis_size(GRP)
    robots, true_steps = actions.shape
    steps = 8
    rows = robots * steps
    prompt_dev, width = key_cache.shape[1:]
    feats, cols = w_query.shape
    bins = embed.shape[0]
    own_bins = head.shape[0]
    lh = cols // HEAD_DIM
    heads = seqs * lh
    n = robots * lh * steps
    scale = HEAD_DIM ** (-0.5)
    bin_ids = jnp.arange(bins, dtype=jnp.int32)
    f32 = jnp.float32
    array = jax.ShapeDtypeStruct

    blocks = w_out[None]
    arrived = from_partner(blocks, "z", 4)
    zs = [0, 4]
    zs = zs + [m ^ 2 for m in zs]
    zs = zs + [m ^ 1 for m in zs]

    acts = jnp.broadcast_to(actions[None], (groups, robots, true_steps))
    acts = exchange(acts, GRP).reshape(groups * robots, true_steps)
    pad_steps = ((0, 0), (0, steps - true_steps))
    acts = jnp.pad(acts, pad_steps).reshape(groups * rows)
    wide = embed.astype(f32)
    mean_square = jnp.mean(wide * wide, axis=-1, keepdims=True)
    part = lax.dynamic_slice(embed, (0, g * feats), (bins, feats)).astype(f32)
    part_gain = lax.dynamic_slice(attn_gain, (g * feats,), (feats,))
    table = (part * lax.rsqrt(mean_square + 1e-05) * part_gain).astype(jnp.bfloat16)
    onehot = (acts[:, None] == bin_ids[None, :]).astype(jnp.bfloat16)
    normed = jnp.dot(onehot, table, preferred_element_type=f32).astype(jnp.bfloat16)
    weights = jnp.concatenate([w_query, w_key, w_value], axis=1)
    terms = jnp.dot(normed, weights, preferred_element_type=f32).astype(jnp.bfloat16)
    terms, lengths, actions, final_gain, head, shard = fenced(
        terms, lengths, actions, final_gain, head, s[None]
    )
    sums = exchange(terms.reshape(groups, rows, 3 * cols), GRP)

    places = (lengths[:, None] + jnp.arange(steps, dtype=jnp.int32)[None, :]).astype(f32)
    half = HEAD_DIM // 2
    freq = 10000.0 ** (-(jnp.arange(half, dtype=f32) * 2.0 / HEAD_DIM))
    angle = places.reshape(rows, 1) * freq
    cosine = jnp.concatenate([jnp.cos(angle)] * 2, axis=1)
    sine = jnp.concatenate([-jnp.sin(angle), jnp.sin(angle)], axis=1)
    prompt_ids = shard[0] * prompt_dev + jnp.arange(prompt_dev, dtype=jnp.int32)
    mask = (prompt_ids[None, :] < lengths[:, None]).astype(f32)
    actions = jnp.pad(actions, pad_steps)
    own_hot = (actions.reshape(rows)[:, None] == bin_ids[None, :]).astype(jnp.bfloat16)
    own_embed = lax.dynamic_slice(embed, (0, s * cols), (bins, cols))
    inputs = jnp.dot(own_hot, own_embed, preferred_element_type=f32)
    own_gain = lax.dynamic_slice(final_gain, (s * cols,), (cols,))[None]
    head_parts = jnp.swapaxes(head.reshape(own_bins, seqs, cols), 0, 1)
    order = (z ^ jnp.array(zs, jnp.int32)) * lax.axis_size("core")
    order = jnp.concatenate([order + core, order + 1 - core])
    blocks = jnp.concatenate([blocks, arrived], axis=0)
    (sums, cosine, sine, mask, inputs, own_gain, head_parts, order, shard, blocks) = fenced(
        sums, cosine, sine, mask, inputs, own_gain, head_parts, order, shard, blocks
    )
    arrived = from_partner(blocks, "z", 2)

    spread, query, key, value = call(
        heads_kernel,
        (array((seqs, rows + own_bins, cols), jnp.bfloat16), *[array((rows, cols), f32)] * 3),
        [in_vmem()] * 4,
        sums,
        cosine,
        sine,
        head_parts,
    )
    spread = exchange(spread, SEQ)
    spread, mask = fenced(spread, mask)
    all_query = spread[:, :rows].reshape(seqs, robots, steps, lh, HEAD_DIM)
    head_cols = spread[:, rows:].reshape(bins, cols)

    mask = (mask > 0.0)[:, None, None, :]
    q = jnp.moveaxis(all_query, 0, 2).reshape(robots, steps, heads, HEAD_DIM)
    cache_keys = key_cache.reshape(robots, prompt_dev, heads, HEAD_DIM)
    cache_values = value_cache.reshape(robots, prompt_dev, heads, HEAD_DIM)
    scores = jnp.einsum("rthd,rphd->rhtp", q, cache_keys, preferred_element_type=f32)
    scores = jnp.where(mask, scores * scale, NEG)
    top = halves(jnp.max(scores, axis=-1))[2]
    e = jnp.where(mask, jnp.exp(scores - top[..., None]), 0.0)
    total = jnp.sum(e, axis=-1)
    acc = jnp.einsum(
        "rhtp,rphd->rhtd", e.astype(jnp.bfloat16), cache_values, preferred_element_type=f32
    )

    def to_owner(x):
        x = x.reshape(robots, seqs, lh, steps, -1)
        return jnp.moveaxis(x, 1, 0).reshape(seqs, n, -1)

    th, tl, _ = halves(to_owner(top)[..., 0])
    lo, ll, _ = halves(to_owner(total)[..., 0])
    stats = jnp.concatenate([th, tl, lo, ll], axis=1)[:, None]
    packed = jnp.concatenate([to_owner(acc.astype(jnp.bfloat16)), stats], axis=1)
    packed, blocks, arrived, head_cols = fenced(packed, blocks, arrived, head_cols)
    blocks = jnp.concatenate([blocks, arrived], axis=0)
    arrived = from_partner(blocks, "z", 1)
    packed = exchange(packed, SEQ)
    attended = call(
        merge_kernel,
        array((seqs, rows, cols), jnp.bfloat16),
        [in_vmem()] * 5,
        query,
        key,
        value,
        packed[:, n],
        packed,
    )
    attended, blocks, arrived = fenced(attended, blocks, arrived)
    blocks = jnp.concatenate([blocks, arrived], axis=0)
    other = from_partner(blocks, "core", 1)

    attended = exchange(attended, SEQ)
    parts = call(
        output_kernel,
        array((seqs, rows, bins), f32),
        [in_smem()] + [in_vmem()] * 6,
        order,
        attended,
        blocks,
        other,
        inputs,
        own_gain,
        head_cols,
    )
    parts = exchange(parts, SEQ)
    return call(
        functools.partial(final_kernel, width=width, steps=steps),
        array((robots, true_steps, own_bins), f32),
        [in_smem(), in_vmem()],
        shard,
        parts,
    )


def solution(mesh):
    torus = Mesh(mesh.devices.reshape(4, 4, 8, 2), ("seq_0", "seq_1", "z", "core"))
    in_specs = (
        P(GRP, None),
        P(GRP),
        P(),
        P(),
        P(GRP, SEQ),
        P(GRP, SEQ),
        P(GRP, SEQ),
        P(GRP, SEQ),
        P(GRP, SEQ, None),
        P(GRP, SEQ, None),
        P(),
        P(SEQ, None),
    )
    out_specs = P(GRP, None, SEQ)

    return jax.shard_map(
        on_device, mesh=torus, in_specs=in_specs, out_specs=out_specs, check_vma=False
    )
```

```python
import functools

import jax
import jax.numpy as jnp
from jax import lax
from jax.experimental import pallas as pl
from jax.experimental.pallas import tpu as pltpu
from jax.sharding import Mesh
from jax.sharding import PartitionSpec as P


HEAD_DIM = 128
SEQ = ("seq_0", "seq_1")
GRP = ("z", "core")
NEG = -1e30


def exchange(pieces, axis):
    return lax.all_to_all(pieces, axis, split_axis=0, concat_axis=0, tiled=True)


def from_partner(x, axis, k):
    return lax.ppermute(x, axis, [(i, i ^ k) for i in range(lax.axis_size(axis))])


def here(x):
    return lax.ppermute(x, "core", [(i, i) for i in range(lax.axis_size("core"))])


def fenced(*arrays):
    return lax.optimization_barrier(arrays)


def in_vmem():
    return pl.BlockSpec(memory_space=pltpu.VMEM)


def in_smem():
    return pl.BlockSpec(memory_space=pltpu.SMEM)


def far():
    return pl.BlockSpec(memory_space=pltpu.HBM)


def call(kernel, out, specs, *args, scratch=(), limit=8):
    outs = (in_vmem(),) * len(out) if isinstance(out, tuple) else in_vmem()
    return pl.pallas_call(
        kernel,
        out_shape=out,
        in_specs=specs,
        out_specs=outs,
        scratch_shapes=scratch,
        compiler_params=pltpu.CompilerParams(vmem_limit_bytes=limit * 2**20),
    )(*args)


def merge_kernel(query, key, value, stats, packed, out):
    seqs, _, head_dim = packed.shape
    rows, cols = query.shape
    lh = cols // head_dim
    steps = 8
    n = rows * lh
    scale = head_dim ** (-0.5)
    causal = lax.broadcasted_iota(jnp.int32, (steps, steps), 1) <= lax.broadcasted_iota(
        jnp.int32, (steps, steps), 0
    )
    tops, totals, accs = [], [], []
    for r in range(rows // steps):
        for h in range(lh):
            at = (slice(r * steps, (r + 1) * steps), slice(h * head_dim, (h + 1) * head_dim))
            q, k, v = (ref[at].astype(jnp.bfloat16) for ref in (query, key, value))
            scores = lax.dot_general(
                q, k, (((1,), (1,)), ((), ())), preferred_element_type=jnp.float32
            )
            scores = jnp.where(causal, scores * scale, NEG)
            top = jnp.max(scores, axis=-1, keepdims=True)
            e = jnp.where(causal, jnp.exp(scores - top), 0.0)
            tops.append(top)
            totals.append(jnp.sum(e, axis=-1, keepdims=True))
            accs.append(jnp.dot(e.astype(jnp.bfloat16), v, preferred_element_type=jnp.float32))
    w_top, w_total, w_acc = (jnp.concatenate(x, axis=0) for x in (tops, totals, accs))
    part = stats[...].astype(jnp.float32)
    part = jnp.concatenate([part, jnp.zeros((4 * n - seqs, 4 * n), jnp.float32)], axis=0).T
    there = lax.broadcasted_iota(jnp.int32, (n, 4 * n), 1) < seqs
    top = jnp.where(there, part[:n] + part[n : 2 * n], NEG)
    total = part[2 * n : 3 * n] + part[3 * n :]
    best = jnp.maximum(jnp.max(top, axis=-1, keepdims=True), w_top)
    factor = jnp.where(there, jnp.exp(top - best), 0.0)
    w_factor = jnp.exp(w_top - best)
    denom = jnp.sum(total * factor, axis=-1, keepdims=True) + w_total * w_factor
    numer = w_acc * w_factor
    for d in range(seqs):
        numer += packed[d, :n, :].astype(jnp.float32) * factor[:, d : d + 1]
    attended = numer / denom
    lines = []
    for r in range(rows // steps):
        own = [attended[(r * lh + h) * steps : (r * lh + h + 1) * steps] for h in range(lh)]
        lines.append(jnp.concatenate(own, axis=1))
    attended = jnp.concatenate(lines, axis=0).astype(jnp.bfloat16)
    for d in range(seqs):
        out[d] = attended


def output_kernel(places, blocks, mine, other, inputs, gain, head, out):
    count = mine.shape[0]
    seqs, rows, _ = blocks.shape
    residual = inputs[...]
    for m in range(count):
        residual += jnp.dot(blocks[places[m]], mine[m], preferred_element_type=jnp.float32)
        residual += jnp.dot(blocks[places[count + m]], other[m], preferred_element_type=jnp.float32)
    gained = (residual * gain[...]).astype(jnp.bfloat16)
    logits = lax.dot_general(
        gained, head[...], (((1,), (1,)), ((), ())), preferred_element_type=jnp.float32
    )
    row = lax.broadcasted_iota(jnp.int32, logits.shape, 0)
    lane = lax.broadcasted_iota(jnp.int32, logits.shape, 1)
    squares = jnp.sum(residual * residual, axis=-1, keepdims=True)
    squares = jnp.sum(jnp.where(row == lane, squares, 0.0), axis=0, keepdims=True)
    result = jnp.where(row == rows - 1, squares, logits)
    for d in range(seqs):
        out[d] = result


def final_kernel(shard, parts, out, *, width, steps):
    seqs, rows, bins = parts.shape
    true_steps, robots, own_bins = out.shape
    total = parts[0]
    for d in range(1, seqs):
        total += parts[d]
    row = lax.broadcasted_iota(jnp.int32, total.shape, 0)
    lane = lax.broadcasted_iota(jnp.int32, total.shape, 1)
    squares = jnp.sum(
        jnp.where(row == lane, total[rows - 1 :], 0.0), axis=-1, keepdims=True
    )
    logits = total * lax.rsqrt(squares / width + 1e-05)
    top = jnp.max(logits, axis=-1, keepdims=True)
    logprob = logits - top - jnp.log(jnp.sum(jnp.exp(logits - top), axis=-1, keepdims=True))
    own = pltpu.roll(logprob, (bins - shard[0] * own_bins) % bins, 1)[:, :own_bins]
    for r in range(robots):
        out[:, r, :] = own[r * steps : r * steps + true_steps]


def parts_of(x):
    high = x.astype(jnp.bfloat16).astype(jnp.float32)
    low = (x - high).astype(jnp.bfloat16).astype(jnp.float32)
    return high, low


def project_kernel(group, shard, acts, own, embed, gain, w_query, w_key, w_value, terms, inputs):
    bins, width = embed.shape
    feats, cols = w_query.shape
    chunk = 512
    squares = jnp.zeros((bins, HEAD_DIM), jnp.float32)
    for c in range(0, width, chunk):
        wide = embed[:, c : c + chunk].astype(jnp.float32)
        wide = wide * wide
        for k in range(0, chunk, HEAD_DIM):
            squares += wide[:, k : k + HEAD_DIM]
    mean_square = jnp.sum(squares, axis=-1, keepdims=True) / width
    here = pl.ds(pl.multiple_of(group[0] * feats, feats), feats)
    part = embed[:, here].astype(jnp.float32)
    lines = feats // HEAD_DIM
    row = jnp.concatenate([gain[pl.ds(group[0] * lines + k, 1)] for k in range(lines)], axis=1)
    table = (part * lax.rsqrt(mean_square + 1e-05) * row).astype(jnp.bfloat16)
    by_bin = lax.broadcasted_iota(jnp.int32, (bins, acts.shape[1]), 0)

    def rows_of(numbers, values):
        hot = jnp.where(by_bin[:, : numbers.shape[1]] == numbers, 1.0, 0.0).astype(jnp.bfloat16)
        return lax.dot_general(
            hot, values, (((0,), (0,)), ((), ())), preferred_element_type=jnp.float32
        )

    normed = rows_of(acts[...], table).astype(jnp.bfloat16)
    for k, w in enumerate((w_query, w_key, w_value)):
        out = jnp.dot(normed, w[...], preferred_element_type=jnp.float32)
        terms[:, k * cols : (k + 1) * cols] = out.astype(jnp.bfloat16)
    there = pl.ds(pl.multiple_of(shard[0] * cols, cols), cols)
    inputs[...] = rows_of(own[...], embed[:, there])[: inputs.shape[0]]


def attend_kernel(shard, lengths, spread, keys_far, values_far, packed, keys, values, sems):
    seqs, _, cols = spread.shape
    robots, prompt_dev, _ = keys.shape
    steps = 8
    n = packed.shape[1] - 8
    scale = HEAD_DIM ** (-0.5)
    group = 2
    copies = []
    for k in range(seqs // group):
        at = slice(k * group * cols, (k + 1) * group * cols)
        copies.append(
            [
                pltpu.make_async_copy(src.at[:, :, at], dst.at[:, :, at], sems.at[i, k])
                for i, (src, dst) in enumerate(((keys_far, keys), (values_far, values)))
            ]
        )
        for copy in copies[-1]:
            copy.start()
    first = lax.broadcasted_iota(jnp.int32, (steps, cols), 1) < HEAD_DIM
    place = lax.broadcasted_iota(jnp.int32, (2 * steps, prompt_dev), 1) + shard[0] * prompt_dev
    block = lax.broadcasted_iota(jnp.int32, (4 * n, HEAD_DIM), 1)
    stats = jnp.zeros((4 * n, HEAD_DIM), jnp.float32)
    for b in range(seqs):
        if b % group == 0:
            for copy in copies[b // group]:
                copy.wait()
        query = spread[b, : robots * steps, :].astype(jnp.float32)
        at = slice(b * cols, (b + 1) * cols)
        columns = []
        for r in range(robots):
            valid = place < lengths[r]
            q = query[r * steps : (r + 1) * steps]
            q = jnp.concatenate([jnp.where(first, q, 0.0), jnp.where(first, 0.0, q)], axis=0)
            scores = lax.dot_general(
                q.astype(jnp.bfloat16),
                keys[r, :, at],
                (((1,), (1,)), ((), ())),
                preferred_element_type=jnp.float32,
            )
            scores = jnp.where(valid, scores * scale, NEG)
            high, low = parts_of(jnp.max(scores, axis=-1, keepdims=True))
            e = jnp.where(valid, jnp.exp(scores - (high + low)), 0.0)
            columns.append((high, low, *parts_of(jnp.sum(e, axis=-1, keepdims=True))))
            acc = jnp.dot(
                e.astype(jnp.bfloat16), values[r, :, at], preferred_element_type=jnp.float32
            )
            acc = jnp.concatenate([acc[:steps, :HEAD_DIM], acc[steps:, HEAD_DIM:]], axis=0)
            packed[b, r * 2 * steps : (r + 1) * 2 * steps, :] = acc.astype(jnp.bfloat16)
        column = jnp.concatenate([columns[r][k] for k in range(4) for r in range(robots)], axis=0)
        stats = jnp.where(block == b, column, stats)
    stats = stats.T.astype(jnp.bfloat16)
    for b in range(seqs):
        packed[b, n:, :] = jnp.broadcast_to(stats[b : b + 1], (8, HEAD_DIM))


def heads_kernel(sums, cosine, sine, head, spread, query, key, value):
    seqs = sums.shape[0]
    cols = query.shape[1]
    rows = query.shape[0]
    total = sums[0].astype(jnp.float32)
    for d in range(1, seqs):
        total += sums[d].astype(jnp.float32)

    def rotated(x):
        parts = []
        for h in range(cols // HEAD_DIM):
            part = x[:, h * HEAD_DIM : (h + 1) * HEAD_DIM]
            turned = pltpu.roll(part, HEAD_DIM // 2, 1)
            parts.append(part * cosine[...] + turned * sine[...])
        return jnp.concatenate(parts, axis=1)

    own = rotated(total[:, :cols])
    query[...] = own
    key[...] = rotated(total[:, cols : 2 * cols])
    value[...] = total[:, 2 * cols :]
    own = own.astype(jnp.bfloat16)
    for d in range(head.shape[0]):
        spread[d, :rows, :] = own
        spread[d, rows:, :] = head[d]


def on_device(
    actions,
    lengths,
    embed,
    attn_gain,
    w_query,
    w_key,
    w_value,
    w_out,
    key_cache,
    value_cache,
    final_gain,
    head,
):
    s = lax.axis_index(SEQ)
    g = lax.axis_index(GRP)
    z = lax.axis_index("z")
    core = lax.axis_index("core")
    seqs = lax.axis_size(SEQ)
    groups = lax.axis_size(GRP)
    robots, true_steps = actions.shape
    steps = 8
    rows = robots * steps
    _, width = key_cache.shape[1:]
    _, cols = w_query.shape
    bins = embed.shape[0]
    own_bins = head.shape[0]
    lh = cols // HEAD_DIM
    n = robots * lh * steps
    f32 = jnp.float32
    array = jax.ShapeDtypeStruct

    near = [here(x) for x in (embed, attn_gain.reshape(-1, HEAD_DIM), w_query, w_key, w_value)]

    blocks = w_out[None]
    arrived = from_partner(blocks, "z", 4)
    zs = [0, 4]
    zs = zs + [m ^ 2 for m in zs]
    zs = zs + [m ^ 1 for m in zs]

    acts = jnp.broadcast_to(actions[None], (groups, robots, true_steps))
    acts = exchange(acts, GRP).reshape(groups * robots, true_steps)
    pad_steps = ((0, 0), (0, steps - true_steps))
    acts = jnp.pad(acts, pad_steps).reshape(1, groups * rows)
    own = jnp.pad(jnp.pad(actions, pad_steps).reshape(1, rows), ((0, 0), (0, HEAD_DIM - rows)))
    terms, inputs = call(
        project_kernel,
        (array((groups * rows, 3 * cols), jnp.bfloat16), array((rows, cols), f32)),
        [in_smem()] * 2 + [in_vmem()] * 7,
        g[None],
        s[None],
        acts,
        own,
        *near,
    )
    terms, lengths, final_gain, head, shard = fenced(terms, lengths, final_gain, head, s[None])
    sums = exchange(terms.reshape(groups, rows, 3 * cols), GRP)

    places = (lengths[:, None] + jnp.arange(steps, dtype=jnp.int32)[None, :]).astype(f32)
    half = HEAD_DIM // 2
    freq = 10000.0 ** (-(jnp.arange(half, dtype=f32) * 2.0 / HEAD_DIM))
    angle = places.reshape(rows, 1) * freq
    cosine = jnp.concatenate([jnp.cos(angle)] * 2, axis=1)
    sine = jnp.concatenate([-jnp.sin(angle), jnp.sin(angle)], axis=1)
    own_gain = lax.dynamic_slice(final_gain, (s * cols,), (cols,))[None]
    head_parts = jnp.swapaxes(head.reshape(own_bins, seqs, cols), 0, 1)
    order = (z ^ jnp.array(zs, jnp.int32)) * lax.axis_size("core")
    order = jnp.concatenate([order + core, order + 1 - core])
    blocks = jnp.concatenate([blocks, arrived], axis=0)
    (sums, cosine, sine, inputs, own_gain, head_parts, order, shard, blocks) = fenced(
        sums, cosine, sine, inputs, own_gain, head_parts, order, shard, blocks
    )
    arrived = from_partner(blocks, "z", 2)

    spread, query, key, value = call(
        heads_kernel,
        (array((seqs, rows + own_bins, cols), jnp.bfloat16), *[array((rows, cols), f32)] * 3),
        [in_vmem()] * 4,
        sums,
        cosine,
        sine,
        head_parts,
    )
    spread = exchange(spread, SEQ)
    head_cols = spread[:, rows:].reshape(bins, cols)

    packed = call(
        attend_kernel,
        array((seqs, n + 8, HEAD_DIM), jnp.bfloat16),
        [in_smem()] * 2 + [in_vmem()] + [far()] * 2,
        shard,
        lengths,
        spread,
        key_cache,
        value_cache,
        scratch=[
            pltpu.VMEM(key_cache.shape, jnp.bfloat16),
            pltpu.VMEM(value_cache.shape, jnp.bfloat16),
            pltpu.SemaphoreType.DMA((2, seqs // 2)),
        ],
        limit=52,
    )
    packed, blocks, arrived, head_cols = fenced(packed, blocks, arrived, head_cols)
    blocks = jnp.concatenate([blocks, arrived], axis=0)
    arrived = from_partner(blocks, "z", 1)
    packed = exchange(packed, SEQ)
    attended = call(
        merge_kernel,
        array((seqs, rows, cols), jnp.bfloat16),
        [in_vmem()] * 5,
        query,
        key,
        value,
        packed[:, n],
        packed,
    )
    attended, blocks, arrived = fenced(attended, blocks, arrived)
    blocks = jnp.concatenate([blocks, arrived], axis=0)
    other = from_partner(blocks, "core", 1)

    attended = exchange(attended, SEQ)
    parts = call(
        output_kernel,
        array((seqs, rows, bins), f32),
        [in_smem()] + [in_vmem()] * 6,
        order,
        attended,
        blocks,
        other,
        inputs,
        own_gain,
        head_cols,
    )
    parts = exchange(parts, SEQ)
    logprob = call(
        functools.partial(final_kernel, width=width, steps=steps),
        array((true_steps, robots, own_bins), f32),
        [in_smem(), in_vmem()],
        shard,
        parts,
    )
    return jnp.swapaxes(logprob, 0, 1)


def solution(mesh):
    torus = Mesh(mesh.devices.reshape(4, 4, 8, 2), ("seq_0", "seq_1", "z", "core"))
    in_specs = (
        P(GRP, None),
        P(GRP),
        P(),
        P(),
        P(GRP, SEQ),
        P(GRP, SEQ),
        P(GRP, SEQ),
        P(GRP, SEQ),
        P(GRP, SEQ, None),
        P(GRP, SEQ, None),
        P(),
        P(SEQ, None),
    )
    out_specs = P(GRP, None, SEQ)

    return jax.shard_map(
        on_device, mesh=torus, in_specs=in_specs, out_specs=out_specs, check_vma=False
    )
```

```python
import functools

import jax
import jax.numpy as jnp
from jax import lax
from jax.experimental import pallas as pl
from jax.experimental.pallas import tpu as pltpu
from jax.sharding import Mesh
from jax.sharding import PartitionSpec as P


HEAD_DIM = 128
SEQ = ("seq_0", "seq_1")
GRP = ("z", "core")
NEG = -1e30


def exchange(pieces, axis):
    return lax.all_to_all(pieces, axis, split_axis=0, concat_axis=0, tiled=True)


def from_partner(x, axis, k):
    return lax.ppermute(x, axis, [(i, i ^ k) for i in range(lax.axis_size(axis))])


def fenced(*arrays):
    return lax.optimization_barrier(arrays)


def in_vmem():
    return pl.BlockSpec(memory_space=pltpu.VMEM)


def in_smem():
    return pl.BlockSpec(memory_space=pltpu.SMEM)


def far():
    return pl.BlockSpec(memory_space=pltpu.HBM)


def call(kernel, out, specs, *args, scratch=(), limit=8):
    outs = (in_vmem(),) * len(out) if isinstance(out, tuple) else in_vmem()
    return pl.pallas_call(
        kernel,
        out_shape=out,
        in_specs=specs,
        out_specs=outs,
        scratch_shapes=scratch,
        compiler_params=pltpu.CompilerParams(vmem_limit_bytes=limit * 2**20),
    )(*args)


def merge_kernel(query, key, value, stats, packed, out):
    seqs, _, head_dim = packed.shape
    rows, cols = query.shape
    lh = cols // head_dim
    steps = 8
    n = rows * lh
    scale = head_dim ** (-0.5)
    causal = lax.broadcasted_iota(jnp.int32, (steps, steps), 1) <= lax.broadcasted_iota(
        jnp.int32, (steps, steps), 0
    )
    tops, totals, accs = [], [], []
    for r in range(rows // steps):
        for h in range(lh):
            at = (slice(r * steps, (r + 1) * steps), slice(h * head_dim, (h + 1) * head_dim))
            q, k, v = (ref[at].astype(jnp.bfloat16) for ref in (query, key, value))
            scores = lax.dot_general(
                q, k, (((1,), (1,)), ((), ())), preferred_element_type=jnp.float32
            )
            scores = jnp.where(causal, scores * scale, NEG)
            top = jnp.max(scores, axis=-1, keepdims=True)
            e = jnp.where(causal, jnp.exp(scores - top), 0.0)
            tops.append(top)
            totals.append(jnp.sum(e, axis=-1, keepdims=True))
            accs.append(jnp.dot(e.astype(jnp.bfloat16), v, preferred_element_type=jnp.float32))
    w_top, w_total, w_acc = (jnp.concatenate(x, axis=0) for x in (tops, totals, accs))
    part = stats[...].astype(jnp.float32)
    part = jnp.concatenate([part, jnp.zeros((4 * n - seqs, 4 * n), jnp.float32)], axis=0).T
    there = lax.broadcasted_iota(jnp.int32, (n, 4 * n), 1) < seqs
    top = jnp.where(there, part[:n] + part[n : 2 * n], NEG)
    total = part[2 * n : 3 * n] + part[3 * n :]
    best = jnp.maximum(jnp.max(top, axis=-1, keepdims=True), w_top)
    factor = jnp.where(there, jnp.exp(top - best), 0.0)
    w_factor = jnp.exp(w_top - best)
    denom = jnp.sum(total * factor, axis=-1, keepdims=True) + w_total * w_factor
    numer = w_acc * w_factor
    for d in range(seqs):
        numer += packed[d, :n, :].astype(jnp.float32) * factor[:, d : d + 1]
    attended = numer / denom
    lines = []
    for r in range(rows // steps):
        own = [attended[(r * lh + h) * steps : (r * lh + h + 1) * steps] for h in range(lh)]
        lines.append(jnp.concatenate(own, axis=1))
    attended = jnp.concatenate(lines, axis=0).astype(jnp.bfloat16)
    for d in range(seqs):
        out[d] = attended


def output_kernel(places, blocks, mine, other, inputs, gain, head, out):
    count = mine.shape[0]
    seqs, rows, _ = blocks.shape
    residual = inputs[...]
    for m in range(count):
        residual += jnp.dot(blocks[places[m]], mine[m], preferred_element_type=jnp.float32)
        residual += jnp.dot(blocks[places[count + m]], other[m], preferred_element_type=jnp.float32)
    gained = (residual * gain[...]).astype(jnp.bfloat16)
    logits = lax.dot_general(
        gained, head[...], (((1,), (1,)), ((), ())), preferred_element_type=jnp.float32
    )
    row = lax.broadcasted_iota(jnp.int32, logits.shape, 0)
    lane = lax.broadcasted_iota(jnp.int32, logits.shape, 1)
    squares = jnp.sum(residual * residual, axis=-1, keepdims=True)
    squares = jnp.sum(jnp.where(row == lane, squares, 0.0), axis=0, keepdims=True)
    result = jnp.where(row == rows - 1, squares, logits)
    for d in range(seqs):
        out[d] = result


def final_kernel(shard, parts, out, *, width, steps):
    seqs, rows, bins = parts.shape
    true_steps, robots, own_bins = out.shape
    total = parts[0]
    for d in range(1, seqs):
        total += parts[d]
    row = lax.broadcasted_iota(jnp.int32, total.shape, 0)
    lane = lax.broadcasted_iota(jnp.int32, total.shape, 1)
    squares = jnp.sum(
        jnp.where(row == lane, total[rows - 1 :], 0.0), axis=-1, keepdims=True
    )
    logits = total * lax.rsqrt(squares / width + 1e-05)
    top = jnp.max(logits, axis=-1, keepdims=True)
    logprob = logits - top - jnp.log(jnp.sum(jnp.exp(logits - top), axis=-1, keepdims=True))
    own = pltpu.roll(logprob, (bins - shard[0] * own_bins) % bins, 1)[:, :own_bins]
    for r in range(robots):
        out[:, r, :] = own[r * steps : r * steps + true_steps]


def parts_of(x):
    high = x.astype(jnp.bfloat16).astype(jnp.float32)
    low = (x - high).astype(jnp.bfloat16).astype(jnp.float32)
    return high, low


def project_kernel(
    group,
    shard,
    acts,
    embed_far,
    gain_far,
    w_query_far,
    w_key_far,
    w_value_far,
    terms,
    inputs,
    embed,
    gain,
    w_query,
    w_key,
    w_value,
    sems,
):
    bins, width = embed.shape
    feats, cols = w_query.shape
    rows = inputs.shape[0]
    chunk = bins // 4
    slabs = [slice(c, c + chunk) for c in range(0, bins, chunk)]
    copies = [(embed_far.at[at], embed.at[at]) for at in slabs]
    copies += [
        (gain_far, gain),
        (w_query_far, w_query),
        (w_key_far, w_key),
        (w_value_far, w_value),
    ]
    copies = [pltpu.make_async_copy(*ends, sems.at[k]) for k, ends in enumerate(copies)]
    for copy in copies:
        copy.start()
    mean_square = []
    for at, copy in zip(slabs, copies):
        copy.wait()
        squares = jnp.zeros((chunk, HEAD_DIM), jnp.float32)
        for k in range(0, width, HEAD_DIM):
            wide = embed[at, k : k + HEAD_DIM].astype(jnp.float32)
            squares += wide * wide
        mean_square.append(jnp.sum(squares, axis=-1, keepdims=True) / width)
    mean_square = jnp.concatenate(mean_square, axis=0)
    for copy in copies[len(slabs) :]:
        copy.wait()
    here = pl.ds(pl.multiple_of(group[0] * feats, feats), feats)
    part = embed[:, here].astype(jnp.float32)
    lines = feats // HEAD_DIM
    row = jnp.concatenate([gain[pl.ds(group[0] * lines + k, 1)] for k in range(lines)], axis=1)
    table = (part * lax.rsqrt(mean_square + 1e-05) * row).astype(jnp.bfloat16)
    by_bin = lax.broadcasted_iota(jnp.int32, (bins, acts.shape[1]), 0)

    def rows_of(numbers, values):
        hot = jnp.where(by_bin[:, : numbers.shape[1]] == numbers, 1.0, 0.0).astype(jnp.bfloat16)
        return lax.dot_general(
            hot, values, (((0,), (0,)), ((), ())), preferred_element_type=jnp.float32
        )

    normed = rows_of(acts[...], table).astype(jnp.bfloat16)
    for k, w in enumerate((w_query, w_key, w_value)):
        out = jnp.dot(normed, w[...], preferred_element_type=jnp.float32)
        terms[:, k * cols : (k + 1) * cols] = out.astype(jnp.bfloat16)
    there = pl.ds(pl.multiple_of(shard[0] * cols, cols), cols)
    count = acts.shape[1]
    own = jnp.broadcast_to(acts[...], (8, count))
    own = pltpu.roll(own, (count - group[0] * rows) % count, 1)[:1, :HEAD_DIM]
    inputs[...] = rows_of(own, embed[:, there])[:rows]


def attend_kernel(shard, lengths, spread, keys_far, values_far, packed, keys, values, sems):
    seqs, _, cols = spread.shape
    robots, prompt_dev, _ = keys.shape
    steps = 8
    n = packed.shape[1] - 8
    scale = HEAD_DIM ** (-0.5)
    chunk = prompt_dev // 4
    copies = []
    for r in range(robots):
        for i, (src, dst) in enumerate(((keys_far, keys), (values_far, values))):
            pieces = [(r, slice(k * chunk, (k + 1) * chunk)) for k in range(4)]
            copies.append(
                [
                    pltpu.make_async_copy(src.at[at], dst.at[at], sems.at[2 * r + i, k])
                    for k, at in enumerate(pieces)
                ]
            )
            for copy in copies[-1]:
                copy.start()
    first = lax.broadcasted_iota(jnp.int32, (steps, cols), 1) < HEAD_DIM
    place = lax.broadcasted_iota(jnp.int32, (2 * steps, prompt_dev), 1) + shard[0] * prompt_dev
    lane = lax.broadcasted_iota(jnp.int32, (2 * steps, HEAD_DIM), 1)
    stats = [[jnp.zeros((2 * steps, HEAD_DIM), jnp.float32)] * 4 for _ in range(robots)]
    for r in range(robots):
        valid = place < lengths[r]
        for copy in copies[2 * r]:
            copy.wait()
        weights = []
        for b in range(seqs):
            at = slice(b * cols, (b + 1) * cols)
            q = spread[b, : robots * steps, :].astype(jnp.float32)[r * steps : (r + 1) * steps]
            q = jnp.concatenate([jnp.where(first, q, 0.0), jnp.where(first, 0.0, q)], axis=0)
            scores = lax.dot_general(
                q.astype(jnp.bfloat16),
                keys[r, :, at],
                (((1,), (1,)), ((), ())),
                preferred_element_type=jnp.float32,
            )
            scores = jnp.where(valid, scores * scale, NEG)
            high, low = parts_of(jnp.max(scores, axis=-1, keepdims=True))
            e = jnp.where(valid, jnp.exp(scores - (high + low)), 0.0)
            columns = (high, low, *parts_of(jnp.sum(e, axis=-1, keepdims=True)))
            stats[r] = [jnp.where(lane == b, c, old) for c, old in zip(columns, stats[r])]
            weights.append(e.astype(jnp.bfloat16))
        for copy in copies[2 * r + 1]:
            copy.wait()
        for b in range(seqs):
            at = slice(b * cols, (b + 1) * cols)
            acc = jnp.dot(weights[b], values[r, :, at], preferred_element_type=jnp.float32)
            acc = jnp.concatenate([acc[:steps, :HEAD_DIM], acc[steps:, HEAD_DIM:]], axis=0)
            packed[b, r * 2 * steps : (r + 1) * 2 * steps, :] = acc.astype(jnp.bfloat16)
    stats = jnp.concatenate([stats[r][k] for k in range(4) for r in range(robots)], axis=0)
    stats = stats.T.astype(jnp.bfloat16)
    for b in range(seqs):
        packed[b, n:, :] = jnp.broadcast_to(stats[b : b + 1], (8, HEAD_DIM))


def heads_kernel(sums, cosine, sine, head, spread, query, key, value):
    seqs = sums.shape[0]
    cols = query.shape[1]
    rows = query.shape[0]
    total = sums[0].astype(jnp.float32)
    for d in range(1, seqs):
        total += sums[d].astype(jnp.float32)

    def rotated(x):
        parts = []
        for h in range(cols // HEAD_DIM):
            part = x[:, h * HEAD_DIM : (h + 1) * HEAD_DIM]
            turned = pltpu.roll(part, HEAD_DIM // 2, 1)
            parts.append(part * cosine[...] + turned * sine[...])
        return jnp.concatenate(parts, axis=1)

    own = rotated(total[:, :cols])
    query[...] = own
    key[...] = rotated(total[:, cols : 2 * cols])
    value[...] = total[:, 2 * cols :]
    own = own.astype(jnp.bfloat16)
    for d in range(head.shape[0]):
        spread[d, :rows, :] = own
        spread[d, rows:, :] = head[d]


def on_device(
    actions,
    lengths,
    embed,
    attn_gain,
    w_query,
    w_key,
    w_value,
    w_out,
    key_cache,
    value_cache,
    final_gain,
    head,
):
    s = lax.axis_index(SEQ)
    g = lax.axis_index(GRP)
    z = lax.axis_index("z")
    core = lax.axis_index("core")
    seqs = lax.axis_size(SEQ)
    groups = lax.axis_size(GRP)
    robots, true_steps = actions.shape
    steps = 8
    rows = robots * steps
    _, width = key_cache.shape[1:]
    feats, cols = w_query.shape
    bins = embed.shape[0]
    own_bins = head.shape[0]
    lh = cols // HEAD_DIM
    n = robots * lh * steps
    f32 = jnp.float32
    array = jax.ShapeDtypeStruct

    blocks = w_out[None]
    arrived = from_partner(blocks, "z", 4)
    zs = [0, 4]
    zs = zs + [m ^ 2 for m in zs]
    zs = zs + [m ^ 1 for m in zs]

    acts = jnp.broadcast_to(actions[None], (groups, robots, true_steps))
    acts = exchange(acts, GRP).reshape(groups * robots, true_steps)
    pad_steps = ((0, 0), (0, steps - true_steps))
    acts = jnp.pad(acts, pad_steps).reshape(1, groups * rows)
    terms, inputs = call(
        project_kernel,
        (array((groups * rows, 3 * cols), jnp.bfloat16), array((rows, cols), f32)),
        [in_smem()] * 2 + [in_vmem()] + [far()] * 5,
        g[None],
        s[None],
        acts,
        embed,
        attn_gain.reshape(-1, HEAD_DIM),
        w_query,
        w_key,
        w_value,
        scratch=[
            pltpu.VMEM((bins, width), jnp.bfloat16),
            pltpu.VMEM((width // HEAD_DIM, HEAD_DIM), f32),
            *[pltpu.VMEM((feats, cols), jnp.bfloat16)] * 3,
            pltpu.SemaphoreType.DMA((8,)),
        ],
        limit=56,
    )
    terms, lengths, final_gain, head, shard = fenced(terms, lengths, final_gain, head, s[None])
    sums = exchange(terms.reshape(groups, rows, 3 * cols), GRP)

    places = (lengths[:, None] + jnp.arange(steps, dtype=jnp.int32)[None, :]).astype(f32)
    half = HEAD_DIM // 2
    freq = 10000.0 ** (-(jnp.arange(half, dtype=f32) * 2.0 / HEAD_DIM))
    angle = places.reshape(rows, 1) * freq
    cosine = jnp.concatenate([jnp.cos(angle)] * 2, axis=1)
    sine = jnp.concatenate([-jnp.sin(angle), jnp.sin(angle)], axis=1)
    own_gain = lax.dynamic_slice(final_gain, (s * cols,), (cols,))[None]
    head_parts = jnp.swapaxes(head.reshape(own_bins, seqs, cols), 0, 1)
    z, core = fenced(z, core, terms)[:2]
    order = (z ^ jnp.array(zs, jnp.int32)) * lax.axis_size("core")
    order = jnp.concatenate([order + core, order + 1 - core])
    blocks = jnp.concatenate([blocks, arrived], axis=0)
    (sums, cosine, sine, inputs, own_gain, head_parts, order, shard, blocks) = fenced(
        sums, cosine, sine, inputs, own_gain, head_parts, order, shard, blocks
    )
    arrived = from_partner(blocks, "z", 2)

    spread, query, key, value = call(
        heads_kernel,
        (array((seqs, rows + own_bins, cols), jnp.bfloat16), *[array((rows, cols), f32)] * 3),
        [in_vmem()] * 4,
        sums,
        cosine,
        sine,
        head_parts,
    )
    spread = exchange(spread, SEQ)
    head_cols = spread[:, rows:].reshape(bins, cols)

    packed = call(
        attend_kernel,
        array((seqs, n + 8, HEAD_DIM), jnp.bfloat16),
        [in_smem()] * 2 + [in_vmem()] + [far()] * 2,
        shard,
        lengths,
        spread,
        key_cache,
        value_cache,
        scratch=[
            pltpu.VMEM(key_cache.shape, jnp.bfloat16),
            pltpu.VMEM(value_cache.shape, jnp.bfloat16),
            pltpu.SemaphoreType.DMA((2 * robots, 4)),
        ],
        limit=52,
    )
    packed, blocks, arrived, head_cols = fenced(packed, blocks, arrived, head_cols)
    blocks = jnp.concatenate([blocks, arrived], axis=0)
    arrived = from_partner(blocks, "z", 1)
    packed = exchange(packed, SEQ)
    attended = call(
        merge_kernel,
        array((seqs, rows, cols), jnp.bfloat16),
        [in_vmem()] * 5,
        query,
        key,
        value,
        packed[:, n],
        packed,
    )
    attended, blocks, arrived = fenced(attended, blocks, arrived)
    blocks = jnp.concatenate([blocks, arrived], axis=0)
    other = from_partner(blocks, "core", 1)

    attended = exchange(attended, SEQ)
    parts = call(
        output_kernel,
        array((seqs, rows, bins), f32),
        [in_smem()] + [in_vmem()] * 6,
        order,
        attended,
        blocks,
        other,
        inputs,
        own_gain,
        head_cols,
    )
    parts = exchange(parts, SEQ)
    logprob = call(
        functools.partial(final_kernel, width=width, steps=steps),
        array((true_steps, robots, own_bins), f32),
        [in_smem(), in_vmem()],
        shard,
        parts,
    )
    return jnp.swapaxes(logprob, 0, 1)


def solution(mesh):
    torus = Mesh(mesh.devices.reshape(4, 4, 8, 2), ("seq_0", "seq_1", "z", "core"))
    in_specs = (
        P(GRP, None),
        P(GRP),
        P(),
        P(),
        P(GRP, SEQ),
        P(GRP, SEQ),
        P(GRP, SEQ),
        P(GRP, SEQ),
        P(GRP, SEQ, None),
        P(GRP, SEQ, None),
        P(),
        P(SEQ, None),
    )
    out_specs = P(GRP, None, SEQ)

    return jax.shard_map(
        on_device, mesh=torus, in_specs=in_specs, out_specs=out_specs, check_vma=False
    )
```

```python
import functools

import jax
import jax.numpy as jnp
from jax import lax
from jax.experimental import pallas as pl
from jax.experimental.pallas import tpu as pltpu
from jax.sharding import Mesh
from jax.sharding import PartitionSpec as P


HEAD_DIM = 128
SEQ = ("seq_0", "seq_1")
GRP = ("z", "core")
NEG = -1e30


def exchange(pieces, axis):
    return lax.all_to_all(pieces, axis, split_axis=0, concat_axis=0, tiled=True)


def from_partner(x, axis, k):
    return lax.ppermute(x, axis, [(i, i ^ k) for i in range(lax.axis_size(axis))])


def fenced(*arrays):
    return lax.optimization_barrier(arrays)


def in_vmem():
    return pl.BlockSpec(memory_space=pltpu.VMEM)


def in_smem():
    return pl.BlockSpec(memory_space=pltpu.SMEM)


def far():
    return pl.BlockSpec(memory_space=pltpu.HBM)


def call(kernel, out, specs, *args, scratch=(), limit=8):
    outs = (in_vmem(),) * len(out) if isinstance(out, tuple) else in_vmem()
    return pl.pallas_call(
        kernel,
        out_shape=out,
        in_specs=specs,
        out_specs=outs,
        scratch_shapes=scratch,
        compiler_params=pltpu.CompilerParams(vmem_limit_bytes=limit * 2**20),
    )(*args)


def merge_kernel(query, key, value, stats, packed, out):
    seqs, _, head_dim = packed.shape
    rows, cols = query.shape
    lh = cols // head_dim
    steps = 8
    n = rows * lh
    scale = head_dim ** (-0.5)
    causal = lax.broadcasted_iota(jnp.int32, (steps, steps), 1) <= lax.broadcasted_iota(
        jnp.int32, (steps, steps), 0
    )
    tops, totals, accs = [], [], []
    for r in range(rows // steps):
        for h in range(lh):
            at = (slice(r * steps, (r + 1) * steps), slice(h * head_dim, (h + 1) * head_dim))
            q, k, v = (ref[at].astype(jnp.bfloat16) for ref in (query, key, value))
            scores = lax.dot_general(
                q, k, (((1,), (1,)), ((), ())), preferred_element_type=jnp.float32
            )
            scores = jnp.where(causal, scores * scale, NEG)
            top = jnp.max(scores, axis=-1, keepdims=True)
            e = jnp.where(causal, jnp.exp(scores - top), 0.0)
            tops.append(top)
            totals.append(jnp.sum(e, axis=-1, keepdims=True))
            accs.append(jnp.dot(e.astype(jnp.bfloat16), v, preferred_element_type=jnp.float32))
    w_top, w_total, w_acc = (jnp.concatenate(x, axis=0) for x in (tops, totals, accs))
    part = stats[...].astype(jnp.float32)
    part = jnp.concatenate([part, jnp.zeros((4 * n - seqs, 4 * n), jnp.float32)], axis=0).T
    there = lax.broadcasted_iota(jnp.int32, (n, 4 * n), 1) < seqs
    top = jnp.where(there, part[:n] + part[n : 2 * n], NEG)
    total = part[2 * n : 3 * n] + part[3 * n :]
    best = jnp.maximum(jnp.max(top, axis=-1, keepdims=True), w_top)
    factor = jnp.where(there, jnp.exp(top - best), 0.0)
    w_factor = jnp.exp(w_top - best)
    denom = jnp.sum(total * factor, axis=-1, keepdims=True) + w_total * w_factor
    numer = w_acc * w_factor
    for d in range(seqs):
        numer += packed[d, :n, :].astype(jnp.float32) * factor[:, d : d + 1]
    attended = numer / denom
    lines = []
    for r in range(rows // steps):
        own = [attended[(r * lh + h) * steps : (r * lh + h + 1) * steps] for h in range(lh)]
        lines.append(jnp.concatenate(own, axis=1))
    attended = jnp.concatenate(lines, axis=0).astype(jnp.bfloat16)
    for d in range(seqs):
        out[d] = attended


def output_kernel(places, blocks, mine, other, inputs, gain, head, out):
    count = mine.shape[0]
    seqs, rows, _ = blocks.shape
    residual = inputs[...]
    for m in range(count):
        residual += jnp.dot(blocks[places[m]], mine[m], preferred_element_type=jnp.float32)
        residual += jnp.dot(blocks[places[count + m]], other[m], preferred_element_type=jnp.float32)
    gained = (residual * gain[...]).astype(jnp.bfloat16)
    logits = lax.dot_general(
        gained, head[...], (((1,), (1,)), ((), ())), preferred_element_type=jnp.float32
    )
    row = lax.broadcasted_iota(jnp.int32, logits.shape, 0)
    lane = lax.broadcasted_iota(jnp.int32, logits.shape, 1)
    squares = jnp.sum(residual * residual, axis=-1, keepdims=True)
    squares = jnp.sum(jnp.where(row == lane, squares, 0.0), axis=0, keepdims=True)
    result = jnp.where(row == rows - 1, squares, logits)
    for d in range(seqs):
        out[d] = result


def final_kernel(shard, parts, out, *, width, steps):
    seqs, rows, bins = parts.shape
    true_steps, robots, own_bins = out.shape
    total = parts[0]
    for d in range(1, seqs):
        total += parts[d]
    row = lax.broadcasted_iota(jnp.int32, total.shape, 0)
    lane = lax.broadcasted_iota(jnp.int32, total.shape, 1)
    squares = jnp.sum(
        jnp.where(row == lane, total[rows - 1 :], 0.0), axis=-1, keepdims=True
    )
    logits = total * lax.rsqrt(squares / width + 1e-05)
    top = jnp.max(logits, axis=-1, keepdims=True)
    logprob = logits - top - jnp.log(jnp.sum(jnp.exp(logits - top), axis=-1, keepdims=True))
    own = pltpu.roll(logprob, (bins - shard[0] * own_bins) % bins, 1)[:, :own_bins]
    for r in range(robots):
        out[:, r, :] = own[r * steps : r * steps + true_steps]


def parts_of(x):
    high = x.astype(jnp.bfloat16).astype(jnp.float32)
    low = (x - high).astype(jnp.bfloat16).astype(jnp.float32)
    return high, low


def table_kernel(group, embed_far, gain_far, table, embed, gain, sems):
    bins, width = embed.shape
    feats = table.shape[1]
    chunk = bins // 4
    slabs = [slice(c, c + chunk) for c in range(0, bins, chunk)]
    copies = [(embed_far.at[at], embed.at[at]) for at in slabs] + [(gain_far, gain)]
    copies = [pltpu.make_async_copy(*ends, sems.at[k]) for k, ends in enumerate(copies)]
    for copy in copies:
        copy.start()
    here = pl.ds(pl.multiple_of(group[0] * feats, feats), feats)
    lines = feats // HEAD_DIM
    copies[-1].wait()
    row = jnp.concatenate([gain[pl.ds(group[0] * lines + k, 1)] for k in range(lines)], axis=1)
    for at, copy in zip(slabs, copies):
        copy.wait()
        squares = jnp.zeros((chunk, HEAD_DIM), jnp.float32)
        for k in range(0, width, HEAD_DIM):
            wide = embed[at, k : k + HEAD_DIM].astype(jnp.float32)
            squares += wide * wide
        mean_square = jnp.sum(squares, axis=-1, keepdims=True) / width
        part = embed[at, here].astype(jnp.float32)
        table[at] = (part * lax.rsqrt(mean_square + 1e-05) * row).astype(jnp.bfloat16)


def project_kernel(acts, table, w_query, w_key, w_value, terms):
    bins, cols = table.shape[0], w_query.shape[1]
    count = acts.shape[1]
    by_bin = lax.broadcasted_iota(jnp.int32, (bins, count), 0)
    hot = jnp.where(by_bin == acts[...], 1.0, 0.0).astype(jnp.bfloat16)
    normed = lax.dot_general(
        hot, table[...], (((0,), (0,)), ((), ())), preferred_element_type=jnp.float32
    ).astype(jnp.bfloat16)
    for k, w in enumerate((w_query, w_key, w_value)):
        out = jnp.dot(normed, w[...], preferred_element_type=jnp.float32)
        terms[:, k * cols : (k + 1) * cols] = out.astype(jnp.bfloat16)


def fetch_kernel(keys_far, keys, sem):
    copy = pltpu.make_async_copy(keys_far.at[0], keys, sem)
    copy.start()
    copy.wait()


def attend_kernel(shard, lengths, spread, early, keys_far, values_far, packed, keys, values, sems):
    seqs, _, cols = spread.shape
    robots, prompt_dev, _ = keys.shape
    steps = 8
    n = packed.shape[1] - 8
    scale = HEAD_DIM ** (-0.5)
    chunk = prompt_dev // 4
    copies = []
    for r in range(robots):
        for i, (src, dst) in enumerate(((keys_far, keys), (values_far, values))):
            if r == 0 and i == 0:
                copies.append([])
                continue
            pieces = [(r, slice(k * chunk, (k + 1) * chunk)) for k in range(4)]
            copies.append(
                [
                    pltpu.make_async_copy(src.at[at], dst.at[at], sems.at[2 * r + i, k])
                    for k, at in enumerate(pieces)
                ]
            )
            for copy in copies[-1]:
                copy.start()
    first = lax.broadcasted_iota(jnp.int32, (steps, cols), 1) < HEAD_DIM
    place = lax.broadcasted_iota(jnp.int32, (2 * steps, prompt_dev), 1) + shard[0] * prompt_dev
    lane = lax.broadcasted_iota(jnp.int32, (2 * steps, HEAD_DIM), 1)
    stats = [[jnp.zeros((2 * steps, HEAD_DIM), jnp.float32)] * 4 for _ in range(robots)]
    for r in range(robots):
        valid = place < lengths[r]
        for copy in copies[2 * r]:
            copy.wait()
        weights = []
        for b in range(seqs):
            at = slice(b * cols, (b + 1) * cols)
            q = spread[b, : robots * steps, :].astype(jnp.float32)[r * steps : (r + 1) * steps]
            q = jnp.concatenate([jnp.where(first, q, 0.0), jnp.where(first, 0.0, q)], axis=0)
            scores = lax.dot_general(
                q.astype(jnp.bfloat16),
                keys[r, :, at] if r else early[:, at],
                (((1,), (1,)), ((), ())),
                preferred_element_type=jnp.float32,
            )
            scores = jnp.where(valid, scores * scale, NEG)
            high, low = parts_of(jnp.max(scores, axis=-1, keepdims=True))
            e = jnp.where(valid, jnp.exp(scores - (high + low)), 0.0)
            columns = (high, low, *parts_of(jnp.sum(e, axis=-1, keepdims=True)))
            stats[r] = [jnp.where(lane == b, c, old) for c, old in zip(columns, stats[r])]
            weights.append(e.astype(jnp.bfloat16))
        for copy in copies[2 * r + 1]:
            copy.wait()
        for b in range(seqs):
            at = slice(b * cols, (b + 1) * cols)
            acc = jnp.dot(weights[b], values[r, :, at], preferred_element_type=jnp.float32)
            acc = jnp.concatenate([acc[:steps, :HEAD_DIM], acc[steps:, HEAD_DIM:]], axis=0)
            packed[b, r * 2 * steps : (r + 1) * 2 * steps, :] = acc.astype(jnp.bfloat16)
    stats = jnp.concatenate([stats[r][k] for k in range(4) for r in range(robots)], axis=0)
    stats = stats.T.astype(jnp.bfloat16)
    for b in range(seqs):
        packed[b, n:, :] = jnp.broadcast_to(stats[b : b + 1], (8, HEAD_DIM))


def heads_kernel(sums, cosine, sine, head, spread, query, key, value):
    seqs = sums.shape[0]
    cols = query.shape[1]
    rows = query.shape[0]
    total = sums[0].astype(jnp.float32)
    for d in range(1, seqs):
        total += sums[d].astype(jnp.float32)

    def rotated(x):
        parts = []
        for h in range(cols // HEAD_DIM):
            part = x[:, h * HEAD_DIM : (h + 1) * HEAD_DIM]
            turned = pltpu.roll(part, HEAD_DIM // 2, 1)
            parts.append(part * cosine[...] + turned * sine[...])
        return jnp.concatenate(parts, axis=1)

    own = rotated(total[:, :cols])
    query[...] = own
    key[...] = rotated(total[:, cols : 2 * cols])
    value[...] = total[:, 2 * cols :]
    own = own.astype(jnp.bfloat16)
    for d in range(head.shape[0]):
        spread[d, :rows, :] = own
        spread[d, rows:, :] = head[d]


def on_device(
    actions,
    lengths,
    embed,
    attn_gain,
    w_query,
    w_key,
    w_value,
    w_out,
    key_cache,
    value_cache,
    final_gain,
    head,
):
    s = lax.axis_index(SEQ)
    g = lax.axis_index(GRP)
    z = lax.axis_index("z")
    core = lax.axis_index("core")
    seqs = lax.axis_size(SEQ)
    groups = lax.axis_size(GRP)
    robots, true_steps = actions.shape
    steps = 8
    rows = robots * steps
    _, width = key_cache.shape[1:]
    feats, cols = w_query.shape
    bins = embed.shape[0]
    own_bins = head.shape[0]
    lh = cols // HEAD_DIM
    n = robots * lh * steps
    f32 = jnp.float32
    array = jax.ShapeDtypeStruct

    blocks = w_out[None]
    arrived = from_partner(blocks, "z", 4)
    zs = [0, 4]
    zs = zs + [m ^ 2 for m in zs]
    zs = zs + [m ^ 1 for m in zs]

    acts = jnp.broadcast_to(actions[None], (groups, robots, true_steps))
    acts = exchange(acts, GRP).reshape(groups * robots, true_steps)
    pad_steps = ((0, 0), (0, steps - true_steps))
    acts = jnp.pad(acts, pad_steps).reshape(1, groups * rows)
    table = call(
        table_kernel,
        array((bins, feats), jnp.bfloat16),
        [in_smem()] + [far()] * 2,
        g[None],
        embed,
        attn_gain.reshape(-1, HEAD_DIM),
        scratch=[
            pltpu.VMEM((bins, width), jnp.bfloat16),
            pltpu.VMEM((width // HEAD_DIM, HEAD_DIM), f32),
            pltpu.SemaphoreType.DMA((5,)),
        ],
        limit=56,
    )
    terms = call(
        project_kernel,
        array((groups * rows, 3 * cols), jnp.bfloat16),
        [in_vmem()] * 5,
        acts,
        table,
        w_query,
        w_key,
        w_value,
        limit=56,
    )
    terms, lengths, final_gain, head, shard, actions, key_cache = fenced(
        terms, lengths, final_gain, head, s[None], actions, key_cache
    )
    sums = exchange(terms.reshape(groups, rows, 3 * cols), GRP)

    places = (lengths[:, None] + jnp.arange(steps, dtype=jnp.int32)[None, :]).astype(f32)
    half = HEAD_DIM // 2
    freq = 10000.0 ** (-(jnp.arange(half, dtype=f32) * 2.0 / HEAD_DIM))
    angle = places.reshape(rows, 1) * freq
    cosine = jnp.concatenate([jnp.cos(angle)] * 2, axis=1)
    sine = jnp.concatenate([-jnp.sin(angle), jnp.sin(angle)], axis=1)
    own = jnp.pad(actions, pad_steps).reshape(rows)
    own = (own[:, None] == jnp.arange(bins, dtype=jnp.int32)[None, :]).astype(jnp.bfloat16)
    own_embed = lax.dynamic_slice(embed, (0, s * cols), (bins, cols))
    inputs = jnp.dot(own, own_embed, preferred_element_type=f32)
    early = call(
        fetch_kernel,
        array(key_cache.shape[1:], key_cache.dtype),
        [far()],
        key_cache,
        scratch=[pltpu.SemaphoreType.DMA(())],
        limit=50,
    )
    own_gain = lax.dynamic_slice(final_gain, (s * cols,), (cols,))[None]
    head_parts = jnp.swapaxes(head.reshape(own_bins, seqs, cols), 0, 1)
    z, core = fenced(z, core, terms)[:2]
    order = (z ^ jnp.array(zs, jnp.int32)) * lax.axis_size("core")
    order = jnp.concatenate([order + core, order + 1 - core])
    blocks = jnp.concatenate([blocks, arrived], axis=0)
    (sums, cosine, sine, inputs, own_gain, head_parts, order, shard, blocks, early) = fenced(
        sums, cosine, sine, inputs, own_gain, head_parts, order, shard, blocks, early
    )
    arrived = from_partner(blocks, "z", 2)

    spread, query, key, value = call(
        heads_kernel,
        (array((seqs, rows + own_bins, cols), jnp.bfloat16), *[array((rows, cols), f32)] * 3),
        [in_vmem()] * 4,
        sums,
        cosine,
        sine,
        head_parts,
    )
    spread = exchange(spread, SEQ)
    head_cols = spread[:, rows:].reshape(bins, cols)

    packed = call(
        attend_kernel,
        array((seqs, n + 8, HEAD_DIM), jnp.bfloat16),
        [in_smem()] * 2 + [in_vmem()] * 2 + [far()] * 2,
        shard,
        lengths,
        spread,
        early,
        key_cache,
        value_cache,
        scratch=[
            pltpu.VMEM(key_cache.shape, jnp.bfloat16),
            pltpu.VMEM(value_cache.shape, jnp.bfloat16),
            pltpu.SemaphoreType.DMA((2 * robots, 4)),
        ],
        limit=50,
    )
    packed, blocks, arrived, head_cols = fenced(packed, blocks, arrived, head_cols)
    blocks = jnp.concatenate([blocks, arrived], axis=0)
    arrived = from_partner(blocks, "z", 1)
    packed = exchange(packed, SEQ)
    attended = call(
        merge_kernel,
        array((seqs, rows, cols), jnp.bfloat16),
        [in_vmem()] * 5,
        query,
        key,
        value,
        packed[:, n],
        packed,
    )
    attended, blocks, arrived = fenced(attended, blocks, arrived)
    blocks = jnp.concatenate([blocks, arrived], axis=0)
    other = from_partner(blocks, "core", 1)

    attended = exchange(attended, SEQ)
    parts = call(
        output_kernel,
        array((seqs, rows, bins), f32),
        [in_smem()] + [in_vmem()] * 6,
        order,
        attended,
        blocks,
        other,
        inputs,
        own_gain,
        head_cols,
    )
    parts = exchange(parts, SEQ)
    logprob = call(
        functools.partial(final_kernel, width=width, steps=steps),
        array((true_steps, robots, own_bins), f32),
        [in_smem(), in_vmem()],
        shard,
        parts,
    )
    return jnp.swapaxes(logprob, 0, 1)


def solution(mesh):
    torus = Mesh(mesh.devices.reshape(4, 4, 8, 2), ("seq_0", "seq_1", "z", "core"))
    in_specs = (
        P(GRP, None),
        P(GRP),
        P(),
        P(),
        P(GRP, SEQ),
        P(GRP, SEQ),
        P(GRP, SEQ),
        P(GRP, SEQ),
        P(GRP, SEQ, None),
        P(GRP, SEQ, None),
        P(),
        P(SEQ, None),
    )
    out_specs = P(GRP, None, SEQ)

    return jax.shard_map(
        on_device, mesh=torus, in_specs=in_specs, out_specs=out_specs, check_vma=False
    )
```

```python
import functools

import jax
import jax.numpy as jnp
from jax import lax
from jax.experimental import pallas as pl
from jax.experimental.pallas import tpu as pltpu
from jax.sharding import Mesh
from jax.sharding import PartitionSpec as P


HEAD_DIM = 128
SEQ = ("seq_0", "seq_1")
GRP = ("z", "core")
NEG = -1e30


def exchange(pieces, axis):
    return lax.all_to_all(pieces, axis, split_axis=0, concat_axis=0, tiled=True)


def from_partner(x, axis, k):
    return lax.ppermute(x, axis, [(i, i ^ k) for i in range(lax.axis_size(axis))])


def fenced(*arrays):
    return lax.optimization_barrier(arrays)


def in_vmem():
    return pl.BlockSpec(memory_space=pltpu.VMEM)


def in_smem():
    return pl.BlockSpec(memory_space=pltpu.SMEM)


def far():
    return pl.BlockSpec(memory_space=pltpu.HBM)


def call(kernel, out, specs, *args, scratch=(), limit=8):
    outs = (in_vmem(),) * len(out) if isinstance(out, tuple) else in_vmem()
    return pl.pallas_call(
        kernel,
        out_shape=out,
        in_specs=specs,
        out_specs=outs,
        scratch_shapes=scratch,
        compiler_params=pltpu.CompilerParams(vmem_limit_bytes=limit * 2**20),
    )(*args)


def merge_kernel(query, key, value, stats, packed, out):
    seqs, _, head_dim = packed.shape
    rows, cols = query.shape
    lh = cols // head_dim
    steps = 8
    n = rows * lh
    scale = head_dim ** (-0.5)
    causal = lax.broadcasted_iota(jnp.int32, (steps, steps), 1) <= lax.broadcasted_iota(
        jnp.int32, (steps, steps), 0
    )
    tops, totals, accs = [], [], []
    for r in range(rows // steps):
        for h in range(lh):
            at = (slice(r * steps, (r + 1) * steps), slice(h * head_dim, (h + 1) * head_dim))
            q, k, v = (ref[at].astype(jnp.bfloat16) for ref in (query, key, value))
            scores = lax.dot_general(
                q, k, (((1,), (1,)), ((), ())), preferred_element_type=jnp.float32
            )
            scores = jnp.where(causal, scores * scale, NEG)
            top = jnp.max(scores, axis=-1, keepdims=True)
            e = jnp.where(causal, jnp.exp(scores - top), 0.0)
            tops.append(top)
            totals.append(jnp.sum(e, axis=-1, keepdims=True))
            accs.append(jnp.dot(e.astype(jnp.bfloat16), v, preferred_element_type=jnp.float32))
    w_top, w_total, w_acc = (jnp.concatenate(x, axis=0) for x in (tops, totals, accs))
    part = stats[...].astype(jnp.float32)
    part = jnp.concatenate([part, jnp.zeros((4 * n - seqs, 4 * n), jnp.float32)], axis=0).T
    there = lax.broadcasted_iota(jnp.int32, (n, 4 * n), 1) < seqs
    top = jnp.where(there, part[:n] + part[n : 2 * n], NEG)
    total = part[2 * n : 3 * n] + part[3 * n :]
    best = jnp.maximum(jnp.max(top, axis=-1, keepdims=True), w_top)
    factor = jnp.where(there, jnp.exp(top - best), 0.0)
    w_factor = jnp.exp(w_top - best)
    denom = jnp.sum(total * factor, axis=-1, keepdims=True) + w_total * w_factor
    numer = w_acc * w_factor
    for d in range(seqs):
        numer += packed[d, :n, :].astype(jnp.float32) * factor[:, d : d + 1]
    attended = numer / denom
    lines = []
    for r in range(rows // steps):
        own = [attended[(r * lh + h) * steps : (r * lh + h + 1) * steps] for h in range(lh)]
        lines.append(jnp.concatenate(own, axis=1))
    attended = jnp.concatenate(lines, axis=0).astype(jnp.bfloat16)
    for d in range(seqs):
        out[d] = attended


def output_kernel(places, blocks, mine, other, inputs, gain, head, out):
    count = mine.shape[0]
    seqs, rows, _ = blocks.shape
    residual = inputs[...]
    for m in range(count):
        residual += jnp.dot(blocks[places[m]], mine[m], preferred_element_type=jnp.float32)
        residual += jnp.dot(blocks[places[count + m]], other[m], preferred_element_type=jnp.float32)
    gained = (residual * gain[...]).astype(jnp.bfloat16)
    logits = lax.dot_general(
        gained, head[...], (((1,), (1,)), ((), ())), preferred_element_type=jnp.float32
    )
    row = lax.broadcasted_iota(jnp.int32, logits.shape, 0)
    lane = lax.broadcasted_iota(jnp.int32, logits.shape, 1)
    squares = jnp.sum(residual * residual, axis=-1, keepdims=True)
    squares = jnp.sum(jnp.where(row == lane, squares, 0.0), axis=0, keepdims=True)
    result = jnp.where(row == rows - 1, squares, logits)
    for d in range(seqs):
        out[d] = result


def final_kernel(shard, parts, out, *, width, steps):
    seqs, rows, bins = parts.shape
    true_steps, robots, own_bins = out.shape
    total = parts[0]
    for d in range(1, seqs):
        total += parts[d]
    row = lax.broadcasted_iota(jnp.int32, total.shape, 0)
    lane = lax.broadcasted_iota(jnp.int32, total.shape, 1)
    squares = jnp.sum(
        jnp.where(row == lane, total[rows - 1 :], 0.0), axis=-1, keepdims=True
    )
    logits = total * lax.rsqrt(squares / width + 1e-05)
    top = jnp.max(logits, axis=-1, keepdims=True)
    logprob = logits - top - jnp.log(jnp.sum(jnp.exp(logits - top), axis=-1, keepdims=True))
    own = pltpu.roll(logprob, (bins - shard[0] * own_bins) % bins, 1)[:, :own_bins]
    for r in range(robots):
        out[:, r, :] = own[r * steps : r * steps + true_steps]


def parts_of(x):
    high = x.astype(jnp.bfloat16).astype(jnp.float32)
    low = (x - high).astype(jnp.bfloat16).astype(jnp.float32)
    return high, low


def table_kernel(group, embed_far, gain_far, table, embed, gain, sems):
    bins, width = embed.shape
    feats = table.shape[1]
    chunk = bins // 4
    slabs = [slice(c, c + chunk) for c in range(0, bins, chunk)]
    copies = [(embed_far.at[at], embed.at[at]) for at in slabs] + [(gain_far, gain)]
    copies = [pltpu.make_async_copy(*ends, sems.at[k]) for k, ends in enumerate(copies)]
    for copy in copies:
        copy.start()
    here = pl.ds(pl.multiple_of(group[0] * feats, feats), feats)
    lines = feats // HEAD_DIM
    copies[-1].wait()
    row = jnp.concatenate([gain[pl.ds(group[0] * lines + k, 1)] for k in range(lines)], axis=1)
    for at, copy in zip(slabs, copies):
        copy.wait()
        squares = jnp.zeros((chunk, HEAD_DIM), jnp.float32)
        for k in range(0, width, HEAD_DIM):
            wide = embed[at, k : k + HEAD_DIM].astype(jnp.float32)
            squares += wide * wide
        mean_square = jnp.sum(squares, axis=-1, keepdims=True) / width
        part = embed[at, here].astype(jnp.float32)
        table[at] = (part * lax.rsqrt(mean_square + 1e-05) * row).astype(jnp.bfloat16)


def project_kernel(core, acts, table, w_query, w_key, w_value, mine, others, terms):
    bins, cols = table.shape[0], w_query.shape[1]
    count = acts.shape[1]
    by_bin = lax.broadcasted_iota(jnp.int32, (bins, count), 0)
    hot = jnp.where(by_bin == acts[...], 1.0, 0.0).astype(jnp.bfloat16)
    normed = lax.dot_general(
        hot, table[...], (((0,), (0,)), ((), ())), preferred_element_type=jnp.float32
    ).astype(jnp.bfloat16)
    for k, w in enumerate((w_query, w_key, w_value)):
        out = jnp.dot(normed, w[...], preferred_element_type=jnp.float32)
        terms[:, k * cols : (k + 1) * cols] = out.astype(jnp.bfloat16)
    rows = 16
    for z in range(count // rows // 2):
        to = slice(z * rows, (z + 1) * rows)
        mine[to] = terms[pl.ds(pl.multiple_of((2 * z + core[0]) * rows, rows), rows)]
        others[to] = terms[pl.ds(pl.multiple_of((2 * z + 1 - core[0]) * rows, rows), rows)]


def fetch_kernel(keys_far, keys, sem):
    copy = pltpu.make_async_copy(keys_far.at[0], keys, sem)
    copy.start()
    copy.wait()


def attend_kernel(shard, lengths, spread, early, keys_far, values_far, packed, keys, values, sems):
    seqs, _, cols = spread.shape
    robots, prompt_dev, _ = keys.shape
    steps = 8
    n = packed.shape[1] - 8
    scale = HEAD_DIM ** (-0.5)
    chunk = prompt_dev // 4
    copies = []
    for r in range(robots):
        for i, (src, dst) in enumerate(((keys_far, keys), (values_far, values))):
            if r == 0 and i == 0:
                copies.append([])
                continue
            pieces = [(r, slice(k * chunk, (k + 1) * chunk)) for k in range(4)]
            copies.append(
                [
                    pltpu.make_async_copy(src.at[at], dst.at[at], sems.at[2 * r + i, k])
                    for k, at in enumerate(pieces)
                ]
            )
            for copy in copies[-1]:
                copy.start()
    first = lax.broadcasted_iota(jnp.int32, (steps, cols), 1) < HEAD_DIM
    place = lax.broadcasted_iota(jnp.int32, (2 * steps, prompt_dev), 1) + shard[0] * prompt_dev
    lane = lax.broadcasted_iota(jnp.int32, (2 * steps, HEAD_DIM), 1)
    stats = [[jnp.zeros((2 * steps, HEAD_DIM), jnp.float32)] * 4 for _ in range(robots)]
    for r in range(robots):
        valid = place < lengths[r]
        for copy in copies[2 * r]:
            copy.wait()
        weights = []
        for b in range(seqs):
            at = slice(b * cols, (b + 1) * cols)
            q = spread[b, : robots * steps, :].astype(jnp.float32)[r * steps : (r + 1) * steps]
            q = jnp.concatenate([jnp.where(first, q, 0.0), jnp.where(first, 0.0, q)], axis=0)
            scores = lax.dot_general(
                q.astype(jnp.bfloat16),
                keys[r, :, at] if r else early[:, at],
                (((1,), (1,)), ((), ())),
                preferred_element_type=jnp.float32,
            )
            scores = jnp.where(valid, scores * scale, NEG)
            high, low = parts_of(jnp.max(scores, axis=-1, keepdims=True))
            e = jnp.where(valid, jnp.exp(scores - (high + low)), 0.0)
            columns = (high, low, *parts_of(jnp.sum(e, axis=-1, keepdims=True)))
            stats[r] = [jnp.where(lane == b, c, old) for c, old in zip(columns, stats[r])]
            weights.append(e.astype(jnp.bfloat16))
        for copy in copies[2 * r + 1]:
            copy.wait()
        for b in range(seqs):
            at = slice(b * cols, (b + 1) * cols)
            acc = jnp.dot(weights[b], values[r, :, at], preferred_element_type=jnp.float32)
            acc = jnp.concatenate([acc[:steps, :HEAD_DIM], acc[steps:, HEAD_DIM:]], axis=0)
            packed[b, r * 2 * steps : (r + 1) * 2 * steps, :] = acc.astype(jnp.bfloat16)
    stats = jnp.concatenate([stats[r][k] for k in range(4) for r in range(robots)], axis=0)
    stats = stats.T.astype(jnp.bfloat16)
    for b in range(seqs):
        packed[b, n:, :] = jnp.broadcast_to(stats[b : b + 1], (8, HEAD_DIM))


def heads_kernel(sums, cosine, sine, head, spread, query, key, value):
    seqs = sums.shape[0]
    cols = query.shape[1]
    rows = query.shape[0]
    total = sums[0].astype(jnp.float32)
    for d in range(1, seqs):
        total += sums[d].astype(jnp.float32)

    def rotated(x):
        parts = []
        for h in range(cols // HEAD_DIM):
            part = x[:, h * HEAD_DIM : (h + 1) * HEAD_DIM]
            turned = pltpu.roll(part, HEAD_DIM // 2, 1)
            parts.append(part * cosine[...] + turned * sine[...])
        return jnp.concatenate(parts, axis=1)

    own = rotated(total[:, :cols])
    query[...] = own
    key[...] = rotated(total[:, cols : 2 * cols])
    value[...] = total[:, 2 * cols :]
    own = own.astype(jnp.bfloat16)
    for d in range(head.shape[0]):
        spread[d, :rows, :] = own
        spread[d, rows:, :] = head[d]


def on_device(
    actions,
    lengths,
    embed,
    attn_gain,
    w_query,
    w_key,
    w_value,
    w_out,
    key_cache,
    value_cache,
    final_gain,
    head,
):
    s = lax.axis_index(SEQ)
    g = lax.axis_index(GRP)
    z = lax.axis_index("z")
    core = lax.axis_index("core")
    seqs = lax.axis_size(SEQ)
    groups = lax.axis_size(GRP)
    depth = lax.axis_size("z")
    robots, true_steps = actions.shape
    steps = 8
    rows = robots * steps
    _, width = key_cache.shape[1:]
    feats, cols = w_query.shape
    bins = embed.shape[0]
    own_bins = head.shape[0]
    lh = cols // HEAD_DIM
    n = robots * lh * steps
    f32 = jnp.float32
    array = jax.ShapeDtypeStruct

    blocks = w_out[None]
    far_block = from_partner(blocks, "z", 4)
    zs = [0, 4]
    zs = zs + [m ^ 2 for m in zs]
    zs = zs + [m ^ 1 for m in zs]

    acts = jnp.broadcast_to(actions[None], (groups, robots, true_steps))
    acts = exchange(acts, GRP).reshape(groups * robots, true_steps)
    pad_steps = ((0, 0), (0, steps - true_steps))
    acts = jnp.pad(acts, pad_steps).reshape(1, groups * rows)
    normalize = lambda *operands: call(
        table_kernel,
        array((bins, feats), jnp.bfloat16),
        [in_smem()] + [far()] * 2,
        *operands,
        scratch=[
            pltpu.VMEM((bins, width), jnp.bfloat16),
            pltpu.VMEM((width // HEAD_DIM, HEAD_DIM), f32),
            pltpu.SemaphoreType.DMA((5,)),
        ],
        limit=56,
    )
    table = normalize(g[None], embed, attn_gain.reshape(-1, HEAD_DIM))
    terms, sent = call(
        project_kernel,
        (array((depth * rows, 3 * cols), jnp.bfloat16),) * 2,
        [in_smem()] + [in_vmem()] * 5,
        core[None],
        acts,
        table,
        w_query,
        w_key,
        w_value,
        scratch=[pltpu.VMEM((groups * rows, 3 * cols), jnp.bfloat16)],
        limit=56,
    )
    arrived = from_partner(sent, "core", 1).astype(f32)
    terms = (terms.astype(f32) + arrived).astype(jnp.bfloat16)
    terms, lengths, final_gain, head, shard, actions, key_cache = fenced(
        terms, lengths, final_gain, head, s[None], actions, key_cache
    )
    sums = exchange(terms.reshape(depth, rows, 3 * cols), "z")

    places = (lengths[:, None] + jnp.arange(steps, dtype=jnp.int32)[None, :]).astype(f32)
    half = HEAD_DIM // 2
    freq = 10000.0 ** (-(jnp.arange(half, dtype=f32) * 2.0 / HEAD_DIM))
    angle = places.reshape(rows, 1) * freq
    cosine = jnp.concatenate([jnp.cos(angle)] * 2, axis=1)
    sine = jnp.concatenate([-jnp.sin(angle), jnp.sin(angle)], axis=1)
    own = jnp.pad(actions, pad_steps).reshape(rows)
    own = (own[:, None] == jnp.arange(bins, dtype=jnp.int32)[None, :]).astype(jnp.bfloat16)
    own_embed = lax.dynamic_slice(embed, (0, s * cols), (bins, cols))
    inputs = jnp.dot(own, own_embed, preferred_element_type=f32)
    fetch = lambda cache: call(
        fetch_kernel,
        array(key_cache.shape[1:], key_cache.dtype),
        [far()],
        cache,
        scratch=[pltpu.SemaphoreType.DMA(())],
        limit=50,
    )
    early = fetch(key_cache)
    own_gain = lax.dynamic_slice(final_gain, (s * cols,), (cols,))[None]
    head_parts = jnp.swapaxes(head.reshape(own_bins, seqs, cols), 0, 1)
    z, core = fenced(z, core, terms)[:2]
    order = (z ^ jnp.array(zs, jnp.int32)) * lax.axis_size("core")
    order = jnp.concatenate([order + core, order + 1 - core])
    blocks = jnp.concatenate([blocks, far_block], axis=0)
    (sums, cosine, sine, inputs, own_gain, head_parts, order, shard, blocks, early) = fenced(
        sums, cosine, sine, inputs, own_gain, head_parts, order, shard, blocks, early
    )
    arrived = from_partner(blocks, "z", 2)

    spread, query, key, value = call(
        heads_kernel,
        (array((seqs, rows + own_bins, cols), jnp.bfloat16), *[array((rows, cols), f32)] * 3),
        [in_vmem()] * 4,
        sums,
        cosine,
        sine,
        head_parts,
    )
    spread = exchange(spread, SEQ)
    head_cols = spread[:, rows:].reshape(bins, cols)

    packed = call(
        attend_kernel,
        array((seqs, n + 8, HEAD_DIM), jnp.bfloat16),
        [in_smem()] * 2 + [in_vmem()] * 2 + [far()] * 2,
        shard,
        lengths,
        spread,
        early,
        key_cache,
        value_cache,
        scratch=[
            pltpu.VMEM(key_cache.shape, jnp.bfloat16),
            pltpu.VMEM(value_cache.shape, jnp.bfloat16),
            pltpu.SemaphoreType.DMA((2 * robots, 4)),
        ],
        limit=50,
    )
    packed, blocks, arrived, head_cols = fenced(packed, blocks, arrived, head_cols)
    blocks = jnp.concatenate([blocks, arrived], axis=0)
    arrived = from_partner(blocks, "z", 1)
    packed = exchange(packed, SEQ)
    attended = call(
        merge_kernel,
        array((seqs, rows, cols), jnp.bfloat16),
        [in_vmem()] * 5,
        query,
        key,
        value,
        packed[:, n],
        packed,
    )
    attended, blocks, arrived = fenced(attended, blocks, arrived)
    blocks = jnp.concatenate([blocks, arrived], axis=0)
    other = from_partner(blocks, "core", 1)

    attended = exchange(attended, SEQ)
    parts = call(
        output_kernel,
        array((seqs, rows, bins), f32),
        [in_smem()] + [in_vmem()] * 6,
        order,
        attended,
        blocks,
        other,
        inputs,
        own_gain,
        head_cols,
    )
    parts = exchange(parts, SEQ)
    logprob = call(
        functools.partial(final_kernel, width=width, steps=steps),
        array((true_steps, robots, own_bins), f32),
        [in_smem(), in_vmem()],
        shard,
        parts,
    )
    return jnp.swapaxes(logprob, 0, 1)


def solution(mesh):
    torus = Mesh(mesh.devices.reshape(4, 4, 8, 2), ("seq_0", "seq_1", "z", "core"))
    in_specs = (
        P(GRP, None),
        P(GRP),
        P(),
        P(),
        P(GRP, SEQ),
        P(GRP, SEQ),
        P(GRP, SEQ),
        P(GRP, SEQ),
        P(GRP, SEQ, None),
        P(GRP, SEQ, None),
        P(),
        P(SEQ, None),
    )
    out_specs = P(GRP, None, SEQ)

    return jax.shard_map(
        on_device, mesh=torus, in_specs=in_specs, out_specs=out_specs, check_vma=False
    )
```

```python
import functools

import jax
import jax.numpy as jnp
from jax import lax
from jax.experimental import pallas as pl
from jax.experimental.pallas import tpu as pltpu
from jax.sharding import Mesh
from jax.sharding import PartitionSpec as P


HEAD_DIM = 128
SEQ = ("seq_0", "seq_1")
GRP = ("z", "core")
NEG = -1e30


def exchange(pieces, axis):
    return lax.all_to_all(pieces, axis, split_axis=0, concat_axis=0, tiled=True)


def from_partner(x, axis, k):
    return lax.ppermute(x, axis, [(i, i ^ k) for i in range(lax.axis_size(axis))])


def fenced(*arrays):
    return lax.optimization_barrier(arrays)


def in_vmem():
    return pl.BlockSpec(memory_space=pltpu.VMEM)


def in_smem():
    return pl.BlockSpec(memory_space=pltpu.SMEM)


def far():
    return pl.BlockSpec(memory_space=pltpu.HBM)


def call(kernel, out, specs, *args, scratch=(), limit=8):
    outs = (in_vmem(),) * len(out) if isinstance(out, tuple) else in_vmem()
    return pl.pallas_call(
        kernel,
        out_shape=out,
        in_specs=specs,
        out_specs=outs,
        scratch_shapes=scratch,
        compiler_params=pltpu.CompilerParams(vmem_limit_bytes=limit * 2**20),
    )(*args)


def merge_kernel(query, key, value, stats, packed, out):
    seqs, _, head_dim = packed.shape
    rows, cols = query.shape
    lh = cols // head_dim
    steps = 8
    n = rows * lh
    scale = head_dim ** (-0.5)
    causal = lax.broadcasted_iota(jnp.int32, (steps, steps), 1) <= lax.broadcasted_iota(
        jnp.int32, (steps, steps), 0
    )
    tops, totals, accs = [], [], []
    for r in range(rows // steps):
        for h in range(lh):
            at = (slice(r * steps, (r + 1) * steps), slice(h * head_dim, (h + 1) * head_dim))
            q, k, v = (ref[at].astype(jnp.bfloat16) for ref in (query, key, value))
            scores = lax.dot_general(
                q, k, (((1,), (1,)), ((), ())), preferred_element_type=jnp.float32
            )
            scores = jnp.where(causal, scores * scale, NEG)
            top = jnp.max(scores, axis=-1, keepdims=True)
            e = jnp.where(causal, jnp.exp(scores - top), 0.0)
            tops.append(top)
            totals.append(jnp.sum(e, axis=-1, keepdims=True))
            accs.append(jnp.dot(e.astype(jnp.bfloat16), v, preferred_element_type=jnp.float32))
    w_top, w_total, w_acc = (jnp.concatenate(x, axis=0) for x in (tops, totals, accs))
    part = stats[...].astype(jnp.float32)
    part = jnp.concatenate([part, jnp.zeros((4 * n - seqs, 4 * n), jnp.float32)], axis=0).T
    there = lax.broadcasted_iota(jnp.int32, (n, 4 * n), 1) < seqs
    top = jnp.where(there, part[:n] + part[n : 2 * n], NEG)
    total = part[2 * n : 3 * n] + part[3 * n :]
    best = jnp.maximum(jnp.max(top, axis=-1, keepdims=True), w_top)
    factor = jnp.where(there, jnp.exp(top - best), 0.0)
    w_factor = jnp.exp(w_top - best)
    denom = jnp.sum(total * factor, axis=-1, keepdims=True) + w_total * w_factor
    numer = w_acc * w_factor
    for d in range(seqs):
        numer += packed[d, :n, :].astype(jnp.float32) * factor[:, d : d + 1]
    attended = numer / denom
    lines = []
    for r in range(rows // steps):
        own = [attended[(r * lh + h) * steps : (r * lh + h + 1) * steps] for h in range(lh)]
        lines.append(jnp.concatenate(own, axis=1))
    attended = jnp.concatenate(lines, axis=0).astype(jnp.bfloat16)
    for d in range(seqs):
        out[d] = attended


def output_kernel(places, blocks, mine, other, inputs, gain, head, out):
    count = mine.shape[0]
    seqs, rows, _ = blocks.shape
    residual = inputs[...]
    for m in range(count):
        residual += jnp.dot(blocks[places[m]], mine[m], preferred_element_type=jnp.float32)
        residual += jnp.dot(blocks[places[count + m]], other[m], preferred_element_type=jnp.float32)
    gained = (residual * gain[...]).astype(jnp.bfloat16)
    logits = lax.dot_general(
        gained, head[...], (((1,), (1,)), ((), ())), preferred_element_type=jnp.float32
    )
    row = lax.broadcasted_iota(jnp.int32, logits.shape, 0)
    lane = lax.broadcasted_iota(jnp.int32, logits.shape, 1)
    squares = jnp.sum(residual * residual, axis=-1, keepdims=True)
    squares = jnp.sum(jnp.where(row == lane, squares, 0.0), axis=0, keepdims=True)
    result = jnp.where(row == rows - 1, squares, logits)
    for d in range(seqs):
        out[d] = result


def final_kernel(shard, parts, out, *, width, steps):
    seqs, rows, bins = parts.shape
    true_steps, robots, own_bins = out.shape
    total = parts[0]
    for d in range(1, seqs):
        total += parts[d]
    row = lax.broadcasted_iota(jnp.int32, total.shape, 0)
    lane = lax.broadcasted_iota(jnp.int32, total.shape, 1)
    squares = jnp.sum(
        jnp.where(row == lane, total[rows - 1 :], 0.0), axis=-1, keepdims=True
    )
    logits = total * lax.rsqrt(squares / width + 1e-05)
    top = jnp.max(logits, axis=-1, keepdims=True)
    logprob = logits - top - jnp.log(jnp.sum(jnp.exp(logits - top), axis=-1, keepdims=True))
    own = pltpu.roll(logprob, (bins - shard[0] * own_bins) % bins, 1)[:, :own_bins]
    for r in range(robots):
        out[:, r, :] = own[r * steps : r * steps + true_steps]


def parts_of(x):
    high = x.astype(jnp.bfloat16).astype(jnp.float32)
    low = (x - high).astype(jnp.bfloat16).astype(jnp.float32)
    return high, low


def table_kernel(group, embed_far, gain_far, table, embed, gain, sems):
    bins, width = embed.shape
    feats = table.shape[1]
    chunk = bins // 4
    slabs = [slice(c, c + chunk) for c in range(0, bins, chunk)]
    copies = [(embed_far.at[at], embed.at[at]) for at in slabs] + [(gain_far, gain)]
    copies = [pltpu.make_async_copy(*ends, sems.at[k]) for k, ends in enumerate(copies)]
    for copy in copies:
        copy.start()
    here = pl.ds(pl.multiple_of(group[0] * feats, feats), feats)
    lines = feats // HEAD_DIM
    copies[-1].wait()
    row = jnp.concatenate([gain[pl.ds(group[0] * lines + k, 1)] for k in range(lines)], axis=1)
    for at, copy in zip(slabs, copies):
        copy.wait()
        squares = jnp.zeros((chunk, HEAD_DIM), jnp.float32)
        for k in range(0, width, HEAD_DIM):
            wide = embed[at, k : k + HEAD_DIM].astype(jnp.float32)
            squares += wide * wide
        mean_square = jnp.sum(squares, axis=-1, keepdims=True) / width
        part = embed[at, here].astype(jnp.float32)
        table[at] = (part * lax.rsqrt(mean_square + 1e-05) * row).astype(jnp.bfloat16)


def project_kernel(core, acts, table, weights, mine, others, terms):
    bins = table.shape[0]
    count = acts.shape[1]
    by_bin = lax.broadcasted_iota(jnp.int32, (bins, count), 0)
    hot = jnp.where(by_bin == acts[...], 1.0, 0.0).astype(jnp.bfloat16)
    normed = lax.dot_general(
        hot, table[...], (((0,), (0,)), ((), ())), preferred_element_type=jnp.float32
    ).astype(jnp.bfloat16)
    out = jnp.dot(normed, weights[...], preferred_element_type=jnp.float32)
    terms[...] = out.astype(jnp.bfloat16)
    rows = 16
    for z in range(count // rows // 2):
        to = slice(z * rows, (z + 1) * rows)
        mine[to] = terms[pl.ds(pl.multiple_of((2 * z + core[0]) * rows, rows), rows)]
        others[to] = terms[pl.ds(pl.multiple_of((2 * z + 1 - core[0]) * rows, rows), rows)]


def fetch_kernel(keys_far, keys, sem):
    copy = pltpu.make_async_copy(keys_far.at[0], keys, sem)
    copy.start()
    copy.wait()


def attend_kernel(shard, lengths, spread, early, keys_far, values_far, packed, keys, values, sems):
    seqs, _, cols = spread.shape
    robots, prompt_dev, _ = keys.shape
    steps = 8
    n = packed.shape[1] - 8
    scale = HEAD_DIM ** (-0.5)
    chunk = prompt_dev // 4
    copies = []
    for r in range(robots):
        for i, (src, dst) in enumerate(((keys_far, keys), (values_far, values))):
            if r == 0 and i == 0:
                copies.append([])
                continue
            pieces = [(r, slice(k * chunk, (k + 1) * chunk)) for k in range(4)]
            copies.append(
                [
                    pltpu.make_async_copy(src.at[at], dst.at[at], sems.at[2 * r + i, k])
                    for k, at in enumerate(pieces)
                ]
            )
            for copy in copies[-1]:
                copy.start()
    first = lax.broadcasted_iota(jnp.int32, (steps, cols), 1) < HEAD_DIM
    place = lax.broadcasted_iota(jnp.int32, (2 * steps, prompt_dev), 1) + shard[0] * prompt_dev
    lane = lax.broadcasted_iota(jnp.int32, (2 * steps, HEAD_DIM), 1)
    stats = [[jnp.zeros((2 * steps, HEAD_DIM), jnp.float32)] * 4 for _ in range(robots)]
    for r in range(robots):
        valid = place < lengths[r]
        for copy in copies[2 * r]:
            copy.wait()
        weights = []
        for b in range(seqs):
            at = slice(b * cols, (b + 1) * cols)
            q = spread[b, : robots * steps, :].astype(jnp.float32)[r * steps : (r + 1) * steps]
            q = jnp.concatenate([jnp.where(first, q, 0.0), jnp.where(first, 0.0, q)], axis=0)
            scores = lax.dot_general(
                q.astype(jnp.bfloat16),
                keys[r, :, at] if r else early[:, at],
                (((1,), (1,)), ((), ())),
                preferred_element_type=jnp.float32,
            )
            scores = jnp.where(valid, scores * scale, NEG)
            high, low = parts_of(jnp.max(scores, axis=-1, keepdims=True))
            e = jnp.where(valid, jnp.exp(scores - (high + low)), 0.0)
            columns = (high, low, *parts_of(jnp.sum(e, axis=-1, keepdims=True)))
            stats[r] = [jnp.where(lane == b, c, old) for c, old in zip(columns, stats[r])]
            weights.append(e.astype(jnp.bfloat16))
        for copy in copies[2 * r + 1]:
            copy.wait()
        for b in range(seqs):
            at = slice(b * cols, (b + 1) * cols)
            acc = jnp.dot(weights[b], values[r, :, at], preferred_element_type=jnp.float32)
            acc = jnp.concatenate([acc[:steps, :HEAD_DIM], acc[steps:, HEAD_DIM:]], axis=0)
            packed[b, r * 2 * steps : (r + 1) * 2 * steps, :] = acc.astype(jnp.bfloat16)
    stats = jnp.concatenate([stats[r][k] for k in range(4) for r in range(robots)], axis=0)
    stats = stats.T.astype(jnp.bfloat16)
    for b in range(seqs):
        packed[b, n:, :] = jnp.broadcast_to(stats[b : b + 1], (8, HEAD_DIM))


def heads_kernel(sums, cosine, sine, head, spread, query, key, value):
    seqs = sums.shape[0]
    cols = query.shape[1]
    rows = query.shape[0]
    total = sums[0].astype(jnp.float32)
    for d in range(1, seqs):
        total += sums[d].astype(jnp.float32)

    def rotated(x):
        parts = []
        for h in range(cols // HEAD_DIM):
            part = x[:, h * HEAD_DIM : (h + 1) * HEAD_DIM]
            turned = pltpu.roll(part, HEAD_DIM // 2, 1)
            parts.append(part * cosine[...] + turned * sine[...])
        return jnp.concatenate(parts, axis=1)

    own = rotated(total[:, :cols])
    query[...] = own
    key[...] = rotated(total[:, cols : 2 * cols])
    value[...] = total[:, 2 * cols :]
    own = own.astype(jnp.bfloat16)
    for d in range(head.shape[0]):
        spread[d, :rows, :] = own
        spread[d, rows:, :] = head[d]


def on_device(
    actions,
    lengths,
    embed,
    attn_gain,
    w_query,
    w_key,
    w_value,
    w_out,
    key_cache,
    value_cache,
    final_gain,
    head,
):
    s = lax.axis_index(SEQ)
    g = lax.axis_index(GRP)
    z = lax.axis_index("z")
    core = lax.axis_index("core")
    seqs = lax.axis_size(SEQ)
    groups = lax.axis_size(GRP)
    depth = lax.axis_size("z")
    robots, true_steps = actions.shape
    steps = 8
    rows = robots * steps
    _, width = key_cache.shape[1:]
    feats, cols = w_query.shape
    bins = embed.shape[0]
    own_bins = head.shape[0]
    lh = cols // HEAD_DIM
    n = robots * lh * steps
    f32 = jnp.float32
    array = jax.ShapeDtypeStruct

    blocks = w_out[None]
    far_block = from_partner(blocks, "z", 4)
    zs = [0, 4]
    zs = zs + [m ^ 2 for m in zs]
    zs = zs + [m ^ 1 for m in zs]

    weights = jnp.concatenate([w_query, w_key, w_value], axis=1)

    acts = jnp.broadcast_to(actions[None], (groups, robots, true_steps))
    acts = exchange(acts, GRP).reshape(groups * robots, true_steps)
    pad_steps = ((0, 0), (0, steps - true_steps))
    acts = jnp.pad(acts, pad_steps).reshape(1, groups * rows)
    normalize = lambda *operands: call(
        table_kernel,
        array((bins, feats), jnp.bfloat16),
        [in_smem()] + [far()] * 2,
        *operands,
        scratch=[
            pltpu.VMEM((bins, width), jnp.bfloat16),
            pltpu.VMEM((width // HEAD_DIM, HEAD_DIM), f32),
            pltpu.SemaphoreType.DMA((5,)),
        ],
        limit=53,
    )
    table = normalize(g[None], embed, attn_gain.reshape(-1, HEAD_DIM))
    terms, sent = call(
        project_kernel,
        (array((depth * rows, 3 * cols), jnp.bfloat16),) * 2,
        [in_smem()] + [in_vmem()] * 3,
        core[None],
        acts,
        table,
        weights,
        scratch=[pltpu.VMEM((groups * rows, 3 * cols), jnp.bfloat16)],
        limit=12,
    )
    arrived = from_partner(sent, "core", 1).astype(f32)
    terms = (terms.astype(f32) + arrived).astype(jnp.bfloat16)
    terms, lengths, final_gain, head, shard, actions, key_cache = fenced(
        terms, lengths, final_gain, head, s[None], actions, key_cache
    )
    sums = exchange(terms.reshape(depth, rows, 3 * cols), "z")

    places = (lengths[:, None] + jnp.arange(steps, dtype=jnp.int32)[None, :]).astype(f32)
    half = HEAD_DIM // 2
    freq = 10000.0 ** (-(jnp.arange(half, dtype=f32) * 2.0 / HEAD_DIM))
    angle = places.reshape(rows, 1) * freq
    cosine = jnp.concatenate([jnp.cos(angle)] * 2, axis=1)
    sine = jnp.concatenate([-jnp.sin(angle), jnp.sin(angle)], axis=1)
    own = jnp.pad(actions, pad_steps).reshape(rows)
    own = (own[:, None] == jnp.arange(bins, dtype=jnp.int32)[None, :]).astype(jnp.bfloat16)
    own_embed = lax.dynamic_slice(embed, (0, s * cols), (bins, cols))
    inputs = jnp.dot(own, own_embed, preferred_element_type=f32)
    fetch = lambda cache: call(
        fetch_kernel,
        array(key_cache.shape[1:], key_cache.dtype),
        [far()],
        cache,
        scratch=[pltpu.SemaphoreType.DMA(())],
        limit=50,
    )
    early = fetch(key_cache)
    own_gain = lax.dynamic_slice(final_gain, (s * cols,), (cols,))[None]
    head_parts = jnp.swapaxes(head.reshape(own_bins, seqs, cols), 0, 1)
    z, core = fenced(z, core, terms)[:2]
    order = (z ^ jnp.array(zs, jnp.int32)) * lax.axis_size("core")
    order = jnp.concatenate([order + core, order + 1 - core])
    blocks = jnp.concatenate([blocks, far_block], axis=0)
    (sums, cosine, sine, inputs, own_gain, head_parts, order, shard, blocks, early) = fenced(
        sums, cosine, sine, inputs, own_gain, head_parts, order, shard, blocks, early
    )
    arrived = from_partner(blocks, "z", 2)

    spread, query, key, value = call(
        heads_kernel,
        (array((seqs, rows + own_bins, cols), jnp.bfloat16), *[array((rows, cols), f32)] * 3),
        [in_vmem()] * 4,
        sums,
        cosine,
        sine,
        head_parts,
    )
    spread = exchange(spread, SEQ)
    head_cols = spread[:, rows:].reshape(bins, cols)

    packed = call(
        attend_kernel,
        array((seqs, n + 8, HEAD_DIM), jnp.bfloat16),
        [in_smem()] * 2 + [in_vmem()] * 2 + [far()] * 2,
        shard,
        lengths,
        spread,
        early,
        key_cache,
        value_cache,
        scratch=[
            pltpu.VMEM(key_cache.shape, jnp.bfloat16),
            pltpu.VMEM(value_cache.shape, jnp.bfloat16),
            pltpu.SemaphoreType.DMA((2 * robots, 4)),
        ],
        limit=50,
    )
    packed, blocks, arrived, head_cols = fenced(packed, blocks, arrived, head_cols)
    blocks = jnp.concatenate([blocks, arrived], axis=0)
    arrived = from_partner(blocks, "z", 1)
    packed = exchange(packed, SEQ)
    attended = call(
        merge_kernel,
        array((seqs, rows, cols), jnp.bfloat16),
        [in_vmem()] * 5,
        query,
        key,
        value,
        packed[:, n],
        packed,
    )
    attended, blocks, arrived = fenced(attended, blocks, arrived)
    blocks = jnp.concatenate([blocks, arrived], axis=0)
    other = from_partner(blocks, "core", 1)

    attended = exchange(attended, SEQ)
    parts = call(
        output_kernel,
        array((seqs, rows, bins), f32),
        [in_smem()] + [in_vmem()] * 6,
        order,
        attended,
        blocks,
        other,
        inputs,
        own_gain,
        head_cols,
    )
    parts = exchange(parts, SEQ)
    logprob = call(
        functools.partial(final_kernel, width=width, steps=steps),
        array((true_steps, robots, own_bins), f32),
        [in_smem(), in_vmem()],
        shard,
        parts,
    )
    return jnp.swapaxes(logprob, 0, 1)


def solution(mesh):
    torus = Mesh(mesh.devices.reshape(4, 4, 8, 2), ("seq_0", "seq_1", "z", "core"))
    in_specs = (
        P(GRP, None),
        P(GRP),
        P(),
        P(),
        P(GRP, SEQ),
        P(GRP, SEQ),
        P(GRP, SEQ),
        P(GRP, SEQ),
        P(GRP, SEQ, None),
        P(GRP, SEQ, None),
        P(),
        P(SEQ, None),
    )
    out_specs = P(GRP, None, SEQ)

    return jax.shard_map(
        on_device, mesh=torus, in_specs=in_specs, out_specs=out_specs, check_vma=False
    )
```
